32 devices in a mesh: dev: 32 (over z, y, x, core).
Axes of the slice: x: 2, y: 2, z: 4, core: 2. Of those that a mesh axis runs over, the one named last changes fastest.
Arguments:
- image_feats: bfloat16 [384, 1152], P('dev'), may hold values from -0.1875 to 0.1875
- text_feats: bfloat16 [384, 1152], P('dev'), may hold values from -0.1875 to 0.1875
- image_head: bfloat16 [1152, 640], replicated, may hold values from -0.1875 to 0.1875
- text_head: bfloat16 [1152, 640], replicated, may hold values from -0.1875 to 0.1875
- log_scale: float32 [], replicated, may hold values from 1.6 to 2.3
- logit_bias: float32 [], replicated, may hold values from -8 to -4
- image_group: int32 [384], P('dev'), may hold values from 0 to 191
- text_group: int32 [384], P('dev'), may hold values from 0 to 191
Outputs:
- loss: float32 [], replicated
- grad_images: bfloat16 [384, 1152], P('dev')
- grad_texts: bfloat16 [384, 1152], P('dev')
- grad_scale: float32 [], replicated
- grad_bias: float32 [], replicated
The draws below stay inside these ranges and needn't reach their ends.
All inputs are finite; a program needn't handle non-finite values.
Results may differ from the reference program's by a relative error of at most 0.0063.
Values may be sent and summed in bfloat16 or wider, within the bound.
No kernel may reach another device: no remote copies, remote signals or barrier semaphores. Data moves between devices by JAX's collectives and lax.ppermute only.
A program may use at most 128 MiB of HBM per device.

```python
import jax
import jax.numpy as jnp
from jax import lax

D = 1152
E = 640
PAIRS = 384


def touch_ends(entries, own_key, low, largest):
    longest = entries.shape.index(max(entries.shape))
    spots = []
    for shift in (0, 1):
        where = [jax.random.randint(jax.random.fold_in(own_key, axis), (), 0, length) for axis, length in enumerate(entries.shape)]
        where[longest] = (where[longest] + shift) % entries.shape[longest]
        spots.append(tuple(where))
    return entries.at[spots[0]].set(low).at[spots[1]].set(largest)


def levels(own_key, extent, shards, low, largest):
    loudness, own = 1.0, jax.random.fold_in(own_key, 6)
    for dim, blocks in shards:
        steps = jnp.exp(jax.random.uniform(jax.random.fold_in(own, dim), (blocks,), jnp.float32, low / len(shards), largest / len(shards)))
        loudness = loudness * jnp.repeat(steps, extent[dim] // blocks).reshape([-1 if axis == dim else 1 for axis in range(len(extent))])
    return loudness


def gaussian(own_key, extent, deviation, reach, shards=(), dtype=jnp.bfloat16):
    gain = levels(own_key, extent, shards, -0.22, 0.18) if shards else 1.0
    array = jax.random.normal(own_key, extent, jnp.float32) * deviation * gain
    return jnp.minimum(jnp.maximum(array, -reach), reach).astype(dtype)


def setup_inputs(seed: int = 0) -> dict:
    streams_of = jax.random.split(jax.random.key(seed), 9)
    image_feats = gaussian(streams_of[0], (PAIRS, D), 0.03, 0.1875, ((0, 32),))
    text_feats = gaussian(streams_of[1], (PAIRS, D), 0.03, 0.1875, ((0, 32),))
    image_head = gaussian(streams_of[2], (D, E), D ** -0.5, 0.1875)
    text_head = gaussian(streams_of[3], (D, E), D ** -0.5, 0.1875)
    log_scale = jnp.clip(jax.random.uniform(streams_of[4], (), jnp.float32, 1.6, 2.3), 1.6, 2.3)
    logit_bias = jnp.clip(jax.random.uniform(streams_of[5], (), jnp.float32, -8.0, -4.0), -8.0, -4.0)
    image_group = touch_ends(jax.random.randint(streams_of[6], (PAIRS,), 0, PAIRS // 2), jax.random.fold_in(streams_of[6], 1), 0, (PAIRS // 2) - 1).astype(jnp.int32)
    text_group = touch_ends(jax.random.randint(streams_of[7], (PAIRS,), 0, PAIRS // 2), jax.random.fold_in(streams_of[7], 1), 0, (PAIRS // 2) - 1).astype(jnp.int32)
    return {"image_feats": image_feats, "text_feats": text_feats, "image_head": image_head, "text_head": text_head, "log_scale": log_scale, "logit_bias": logit_bias, "image_group": image_group, "text_group": text_group}


epsilon = 1e-06

def normalize(projected):
    length = jnp.sqrt(lax.optimization_barrier(jnp.sum(projected * projected, axis=1, keepdims=True)) + epsilon)
    return (projected / length, length)

def backward_rows(grad_unit, unit_vec, length, weights):
    inner = lax.optimization_barrier(jnp.sum(unit_vec * grad_unit, axis=1, keepdims=True))
    grad_proj = ((grad_unit - unit_vec * inner) / length).astype(jnp.bfloat16)
    return jnp.dot(grad_proj, weights.T, preferred_element_type=jnp.float32).astype(jnp.bfloat16)

def reference(image_feats, text_feats, image_head, text_head, log_scale, logit_bias, image_group, text_group):
    img_unit, img_length = normalize(jnp.dot(image_feats, image_head, preferred_element_type=jnp.float32))
    txt_unit, txt_length = normalize(jnp.dot(text_feats, text_head, preferred_element_type=jnp.float32))
    img_emb = img_unit.astype(jnp.bfloat16)
    txt_emb = txt_unit.astype(jnp.bfloat16)
    logit_scale = jnp.exp(log_scale)
    cosine = jnp.dot(img_emb, txt_emb.T, preferred_element_type=jnp.float32)
    label_sign = jnp.where(image_group[:, None] == text_group[None, :], 1.0, -1.0).astype(jnp.float32)
    margin = label_sign * (logit_scale * cosine + logit_bias)
    total = jnp.sum(jax.nn.softplus(-margin))
    slopes = -label_sign * jax.nn.sigmoid(-margin)
    slope_low = slopes.astype(jnp.bfloat16)
    grad_img_unit = logit_scale * jnp.dot(slope_low, txt_emb, preferred_element_type=jnp.float32)
    grad_txt_unit = logit_scale * jnp.dot(slope_low.T, img_emb, preferred_element_type=jnp.float32)
    pairs = image_feats.shape[0]
    loss = total / pairs
    grad_scale = logit_scale * jnp.sum(slopes * cosine) / pairs
    grad_bias = jnp.sum(slopes) / pairs
    grad_images = backward_rows(grad_img_unit, img_unit, img_length, image_head)
    grad_texts = backward_rows(grad_txt_unit, txt_unit, txt_length, text_head)
    return (loss, grad_images, grad_texts, grad_scale, grad_bias)
```

```python
import functools

import jax
import jax.numpy as jnp
from jax import lax
from jax.experimental import pallas as pl
from jax.experimental.pallas import tpu as pltpu
from jax.sharding import PartitionSpec as P

epsilon = 1e-06
LANES = 128
BITS = 32
LOGIT_BUDGET = 4 << 20


def normalize(projected):
    length = jnp.sqrt(jnp.sum(projected * projected, axis=1, keepdims=True) + epsilon)
    return (projected / length, length)


def contract_last(a, b):
    return lax.dot_general(a, b, (((1,), (1,)), ((), ())), preferred_element_type=jnp.float32)


def backward_rows(grad_unit, unit_vec, length, weights):
    inner = jnp.sum(unit_vec * grad_unit, axis=1, keepdims=True)
    grad_proj = ((grad_unit - unit_vec * inner) / length).astype(jnp.bfloat16)
    return contract_last(grad_proj, weights).astype(jnp.bfloat16)


def on_device_large(
    image_feats, text_feats, image_head, text_head, log_scale, logit_bias, image_group, text_group
):
    img_unit, img_length = normalize(
        jnp.dot(image_feats, image_head, preferred_element_type=jnp.float32)
    )
    txt_unit, txt_length = normalize(
        jnp.dot(text_feats, text_head, preferred_element_type=jnp.float32)
    )
    img_emb = img_unit.astype(jnp.bfloat16)
    txt_emb = txt_unit.astype(jnp.bfloat16)
    logit_scale = jnp.exp(log_scale)
    pairs = image_feats.shape[0] * lax.axis_size("dev")
    emb_piece = lax.all_gather(jnp.stack([img_emb, txt_emb]), "dev", axis=1, tiled=True)
    id_piece = lax.all_gather(jnp.stack([image_group, text_group]), "dev", axis=1, tiled=True)

    def side(emb, others, group, other_group):
        cosine = contract_last(emb, others)
        label = jnp.where(group[:, None] == other_group[None, :], 1.0, -1.0).astype(jnp.float32)
        margin = label * (logit_scale * cosine + logit_bias)
        slopes = -label * jax.nn.sigmoid(-margin)
        grad = logit_scale * jnp.dot(
            slopes.astype(jnp.bfloat16), others, preferred_element_type=jnp.float32
        )
        return cosine, margin, slopes, grad

    cosine, margin, slopes, grad_img = side(img_emb, emb_piece[1], image_group, id_piece[1])
    local_sums = jnp.stack(
        [jnp.sum(jax.nn.softplus(-margin)), jnp.sum(slopes * cosine), jnp.sum(slopes)]
    )
    grad_txt = side(txt_emb, emb_piece[0], text_group, id_piece[0])[3]
    totals = lax.psum(local_sums, "dev")
    return (
        totals[0] / pairs,
        backward_rows(grad_img, img_unit, img_length, image_head),
        backward_rows(grad_txt, txt_unit, txt_length, text_head),
        logit_scale * totals[1] / pairs,
        totals[2] / pairs,
    )


def project_kernel(
    image_ids, text_ids, image_feats, text_feats, image_head, text_head,
    payload, img_unit, txt_unit, img_length, txt_length, image_kept, text_kept,
    frame, sems,
):
    rows, width = img_unit.shape
    odd = lax.rem(lax.axis_index("dev"), 2) == 1
    copies = [
        pltpu.make_async_copy(image_head, image_kept, sems.at[0]),
        pltpu.make_async_copy(text_head, text_kept, sems.at[1]),
    ]
    for copy in copies:
        copy.start()

    position = lax.broadcasted_iota(jnp.int32, (2 * rows, LANES), 0)
    bit = lax.broadcasted_iota(jnp.int32, (2 * rows, LANES), 1)
    ids = jnp.zeros((2 * rows, LANES), jnp.int32)
    for row in range(rows):
        image_id, text_id = image_ids[row], text_ids[row]
        ids = jnp.where(position == row, jnp.where(odd, text_id, image_id), ids)
        ids = jnp.where(position == rows + row, jnp.where(odd, image_id, text_id), ids)
    signs = jnp.where((lax.shift_right_logical(ids, bit & (BITS - 1)) & 1) == 1, 1.0, -1.0)
    payload[width // LANES] = jnp.where(bit < BITS, signs, 0.0).astype(jnp.bfloat16)

    units = []
    sides = (
        (image_feats, image_kept, img_unit, img_length),
        (text_feats, text_kept, txt_unit, txt_length),
    )
    for copy, (feats, kept, unit_out, length_out) in zip(copies, sides):
        copy.wait()
        unit, length = normalize(
            jnp.dot(feats[...], kept[...], preferred_element_type=jnp.float32)
        )
        unit_out[...] = unit
        length_out[...] = jnp.broadcast_to(length, length_out.shape)
        units.append(unit)
    frame[:rows] = jnp.where(odd, units[1], units[0])
    frame[rows:] = jnp.where(odd, units[0], units[1])
    for block in range(width // LANES):
        columns = slice(block * LANES, (block + 1) * LANES)
        payload[block] = frame[:, columns].astype(jnp.bfloat16)


def pair_terms(cosine, matches, scale, bias):
    label = jnp.where(matches > BITS - 1.0, 1.0, -1.0)
    negative = -label * (scale * cosine + bias)
    decay = jnp.exp(-jnp.abs(negative))
    inverse = 1.0 / (1.0 + decay)
    slopes = -label * jnp.where(negative >= 0.0, inverse, decay * inverse)
    return negative, decay, slopes


def loss_kernel(
    chips, pairs,
    log_scale, logit_bias, mine, other, own, img_unit, txt_unit, img_length, txt_length,
    image_head, text_head,
    loss, grad_images, grad_texts, grad_scale, grad_bias,
    img_all, txt_all,
):
    rows, width = img_unit.shape
    frame_rows = 2 * rows
    blocks = width // LANES + 1
    device = lax.axis_index("dev")
    odd, chip = lax.rem(device, 2), device // 2
    depth = chips.bit_length() - 1
    scale = jnp.exp(jnp.full((1, 1), log_scale[0], jnp.float32))
    bias = logit_bias[0]

    position = lax.broadcasted_iota(jnp.int32, (frame_rows, LANES), 0)
    from_mine = (position < rows) == (odd == 0)
    for target in range(chips):
        apart = jnp.bitwise_xor(chip, target)
        slot = 0
        for level in range(depth):
            slot += ((apart >> level) & 1) << (depth - 1 - level)
        at = slice(target * frame_rows, (target + 1) * frame_rows)
        for block in range(blocks):
            a = mine[slot, block].astype(jnp.float32)
            b = other[slot, block].astype(jnp.float32)
            columns = slice(block * LANES, (block + 1) * LANES)
            img_all[at, columns] = jnp.where(from_mine, a, b).astype(jnp.bfloat16)
            txt_all[at, columns] = jnp.where(from_mine, b, a).astype(jnp.bfloat16)

    img_ids, txt_ids = img_all[:, width:], txt_all[:, width:]
    cosine = contract_last(img_all[:, :width], txt_all[:, :width])
    negative, decay, slopes = pair_terms(cosine, contract_last(img_ids, txt_ids), scale, bias)
    total = jnp.sum(jnp.maximum(negative, 0.0) + jnp.log1p(decay), keepdims=True)
    loss[0] = (total / pairs)[0, 0]
    grad_scale[0] = (scale * jnp.sum(slopes * cosine, keepdims=True) / pairs)[0, 0]
    grad_bias[0] = (jnp.sum(slopes, keepdims=True) / pairs)[0, 0]

    ids = own[blocks - 1].astype(jnp.float32)
    top, bottom = ids[:rows], ids[rows:]
    img_own_ids = jnp.where(odd == 0, top, bottom).astype(jnp.bfloat16)
    txt_own_ids = jnp.where(odd == 0, bottom, top).astype(jnp.bfloat16)
    sides = (
        (img_unit, img_length, img_own_ids, txt_all, txt_ids, image_head, grad_images),
        (txt_unit, txt_length, txt_own_ids, img_all, img_ids, text_head, grad_texts),
    )
    for unit_ref, length_ref, own_ids, others, other_ids, head, out in sides:
        unit = unit_ref[...]
        near = contract_last(unit.astype(jnp.bfloat16), others[:, :width])
        slopes = pair_terms(near, contract_last(own_ids, other_ids), scale, bias)[2]
        grad = scale * jnp.dot(
            slopes.astype(jnp.bfloat16), others[:, :width], preferred_element_type=jnp.float32
        )
        out[...] = backward_rows(grad, unit, length_ref[:, :1], head[...])


def on_device_small(
    image_feats, text_feats, image_head, text_head, log_scale, logit_bias, image_group, text_group
):
    devices = lax.axis_size("dev")
    chips = devices // 2
    rows, depth = image_feats.shape
    width = image_head.shape[1]
    blocks = width // LANES + 1
    vmem, smem, hbm = (
        pl.BlockSpec(memory_space=pltpu.VMEM),
        pl.BlockSpec(memory_space=pltpu.SMEM),
        pl.BlockSpec(memory_space=pl.ANY),
    )
    f32, bf16 = jnp.float32, jnp.bfloat16
    payload, img_unit, txt_unit, img_length, txt_length, image_kept, text_kept = pl.pallas_call(
        project_kernel,
        out_shape=(
            jax.ShapeDtypeStruct((blocks, 2 * rows, LANES), bf16),
            jax.ShapeDtypeStruct((rows, width), f32),
            jax.ShapeDtypeStruct((rows, width), f32),
            jax.ShapeDtypeStruct((rows, LANES), f32),
            jax.ShapeDtypeStruct((rows, LANES), f32),
            jax.ShapeDtypeStruct((depth, width), bf16),
            jax.ShapeDtypeStruct((depth, width), bf16),
        ),
        in_specs=[smem, smem, vmem, vmem, hbm, hbm],
        out_specs=(vmem,) * 7,
        scratch_shapes=[pltpu.VMEM((2 * rows, width), f32), pltpu.SemaphoreType.DMA((2,))],
        compiler_params=pltpu.CompilerParams(vmem_limit_bytes=16 << 20),
        name="project",
    )(image_group, text_group, image_feats, text_feats, image_head, text_head)

    def exchange(array, mask):
        return lax.ppermute(array, "dev", [(i, i ^ mask) for i in range(devices)])

    mine = payload[None]
    mask = devices // 2
    while mask > 1:
        mine = jnp.concatenate([mine, exchange(mine, mask)], axis=0)
        mask //= 2
    other = exchange(mine, 1)

    loss, grad_images, grad_texts, grad_scale, grad_bias = pl.pallas_call(
        functools.partial(loss_kernel, chips, rows * devices),
        out_shape=(
            jax.ShapeDtypeStruct((1,), f32),
            jax.ShapeDtypeStruct((rows, depth), bf16),
            jax.ShapeDtypeStruct((rows, depth), bf16),
            jax.ShapeDtypeStruct((1,), f32),
            jax.ShapeDtypeStruct((1,), f32),
        ),
        in_specs=[smem, smem] + [vmem] * 9,
        out_specs=(smem, vmem, vmem, smem, smem),
        scratch_shapes=[pltpu.VMEM((rows * devices, blocks * LANES), bf16)] * 2,
        compiler_params=pltpu.CompilerParams(vmem_limit_bytes=24 << 20),
        name="loss",
    )(
        log_scale.reshape(1), logit_bias.reshape(1), mine, other, payload,
        img_unit, txt_unit, img_length, txt_length, image_kept, text_kept,
    )
    return (loss[0], grad_images, grad_texts, grad_scale[0], grad_bias[0])


def on_device(image_feats, text_feats, image_head, *rest):
    devices = lax.axis_size("dev")
    pairs = image_feats.shape[0] * devices
    small = (
        4 * pairs * pairs <= LOGIT_BUDGET
        and devices >= 4
        and devices & (devices - 1) == 0
        and image_head.shape[1] % LANES == 0
    )
    body = on_device_small if small else on_device_large
    return body(image_feats, text_feats, image_head, *rest)


def solution(mesh):
    placed = (P("dev", None), P("dev", None), P(), P(), P(), P(), P("dev"), P("dev"))
    return jax.shard_map(
        on_device,
        mesh=mesh,
        in_specs=placed,
        out_specs=(P(), P("dev", None), P("dev", None), P(), P()),
        check_vma=False,
    )
```

```python
import functools

import jax
import jax.numpy as jnp
from jax import lax
from jax.experimental import pallas as pl
from jax.experimental.pallas import tpu as pltpu
from jax.sharding import PartitionSpec as P

epsilon = 1e-06
LANES = 128
TILE = 8
BITS = 32
LOGIT_BUDGET = 4 << 20


def normalize(projected):
    length = jnp.sqrt(jnp.sum(projected * projected, axis=1, keepdims=True) + epsilon)
    return (projected / length, length)


def contract_last(a, b):
    return lax.dot_general(a, b, (((1,), (1,)), ((), ())), preferred_element_type=jnp.float32)


def backward_rows(grad_unit, unit_vec, length, weights):
    inner = jnp.sum(unit_vec * grad_unit, axis=1, keepdims=True)
    grad_proj = ((grad_unit - unit_vec * inner) / length).astype(jnp.bfloat16)
    return contract_last(grad_proj, weights).astype(jnp.bfloat16)


def on_device_large(
    image_feats, text_feats, image_head, text_head, log_scale, logit_bias, image_group, text_group
):
    img_unit, img_length = normalize(
        jnp.dot(image_feats, image_head, preferred_element_type=jnp.float32)
    )
    txt_unit, txt_length = normalize(
        jnp.dot(text_feats, text_head, preferred_element_type=jnp.float32)
    )
    img_emb = img_unit.astype(jnp.bfloat16)
    txt_emb = txt_unit.astype(jnp.bfloat16)
    logit_scale = jnp.exp(log_scale)
    pairs = image_feats.shape[0] * lax.axis_size("dev")
    emb_piece = lax.all_gather(jnp.stack([img_emb, txt_emb]), "dev", axis=1, tiled=True)
    id_piece = lax.all_gather(jnp.stack([image_group, text_group]), "dev", axis=1, tiled=True)

    def side(emb, others, group, other_group):
        cosine = contract_last(emb, others)
        label = jnp.where(group[:, None] == other_group[None, :], 1.0, -1.0).astype(jnp.float32)
        margin = label * (logit_scale * cosine + logit_bias)
        slopes = -label * jax.nn.sigmoid(-margin)
        grad = logit_scale * jnp.dot(
            slopes.astype(jnp.bfloat16), others, preferred_element_type=jnp.float32
        )
        return cosine, margin, slopes, grad

    cosine, margin, slopes, grad_img = side(img_emb, emb_piece[1], image_group, id_piece[1])
    local_sums = jnp.stack(
        [jnp.sum(jax.nn.softplus(-margin)), jnp.sum(slopes * cosine), jnp.sum(slopes)]
    )
    grad_txt = side(txt_emb, emb_piece[0], text_group, id_piece[0])[3]
    totals = lax.psum(local_sums, "dev")
    return (
        totals[0] / pairs,
        backward_rows(grad_img, img_unit, img_length, image_head),
        backward_rows(grad_txt, txt_unit, txt_length, text_head),
        logit_scale * totals[1] / pairs,
        totals[2] / pairs,
    )


def project_kernel(
    image_ids, text_ids, image_feats, text_feats, image_head, text_head,
    payload, img_kept, txt_kept,
    image_kept, text_kept, frame, image_rows, text_rows, image_marks, text_marks, head_sems, sems,
):
    rows, width = image_feats.shape[0], image_head.shape[1]
    depth, chunks = image_head.shape[0], head_sems.shape[1]
    step = depth // chunks
    odd = lax.rem(lax.axis_index("dev"), 2) == 1
    small = [
        pltpu.make_async_copy(source, target, sems.at[i])
        for i, (source, target) in enumerate(
            (
                (image_feats, image_rows),
                (text_feats, text_rows),
                (image_ids, image_marks),
                (text_ids, text_marks),
            )
        )
    ]
    large = [
        [
            pltpu.make_async_copy(
                head.at[pl.ds(i * step, step)], kept.at[pl.ds(i * step, step)], head_sems.at[side, i]
            )
            for i in range(chunks)
        ]
        for side, (head, kept) in enumerate(((image_head, image_kept), (text_head, text_kept)))
    ]
    small[0].start()
    for copy in large[0]:
        copy.start()
    for copy in small[1:]:
        copy.start()
    for copy in large[1]:
        copy.start()

    units = []
    sides = (
        (image_rows, image_kept, img_kept),
        (text_rows, text_kept, txt_kept),
    )
    for side, (feats, kept, out) in enumerate(sides):
        small[side].wait()
        projected = jnp.zeros((rows, width), jnp.float32)
        for i, copy in enumerate(large[side]):
            copy.wait()
            part = slice(i * step, (i + 1) * step)
            projected += jnp.dot(feats[:, part], kept[part], preferred_element_type=jnp.float32)
        unit, length = normalize(projected)
        out[:, :width] = unit
        out[:, width:] = jnp.broadcast_to(length, (rows, LANES))
        units.append(unit)
    frame[:rows] = jnp.where(odd, units[1], units[0])
    frame[rows:] = jnp.where(odd, units[0], units[1])
    groups = 2 * rows // TILE
    for block in range(width // LANES):
        columns = slice(block * LANES, (block + 1) * LANES)
        for group in range(groups):
            part = frame[group * TILE : (group + 1) * TILE, columns]
            payload[block * groups + group] = part.astype(jnp.bfloat16)

    small[2].wait()
    small[3].wait()
    position = lax.broadcasted_iota(jnp.int32, (TILE, LANES), 0)
    lane = lax.broadcasted_iota(jnp.int32, (TILE, LANES), 1)
    position += TILE * (lane // BITS)
    ids = jnp.zeros((TILE, LANES), jnp.int32)
    for row in range(rows):
        image_id, text_id = image_marks[row], text_marks[row]
        ids = jnp.where(position == row, jnp.where(odd, text_id, image_id), ids)
        ids = jnp.where(position == rows + row, jnp.where(odd, image_id, text_id), ids)
    bits = lax.shift_right_logical(ids, lane & (BITS - 1)) & 1
    payload[payload.shape[0] - 1] = jnp.where(bits == 1, 1.0, -1.0).astype(jnp.bfloat16)


def frame_of(ref, slot, block, groups, lane):
    if (block + 1) * groups < ref.shape[1]:
        tiles = ref[slot, block * groups : (block + 1) * groups].astype(jnp.float32)
        return tiles.reshape(groups * TILE, LANES)
    packed = ref[slot, ref.shape[1] - 1].astype(jnp.float32)
    turned = [packed] + [
        pltpu.roll(packed, LANES - group * BITS, axis=1) for group in range(1, groups)
    ]
    return jnp.where(lane < BITS, jnp.concatenate(turned, axis=0), 0.0)


def pair_terms(cosine, matches, scale, bias):
    label = jnp.where(matches > BITS - 1.0, 1.0, -1.0)
    negative = -label * (scale * cosine + bias)
    decay = jnp.exp(-jnp.abs(negative))
    inverse = 1.0 / (1.0 + decay)
    slopes = -label * jnp.where(negative >= 0.0, inverse, decay * inverse)
    return negative, decay, slopes


def loss_kernel(
    chips, pairs,
    log_scale, logit_bias, near, far, near_other, far_other, img_kept, txt_kept,
    image_head, text_head,
    loss, grad_images, grad_texts, grad_scale, grad_bias,
    img_frames, txt_frames, image_held, text_held, sems,
):
    rows, width = img_kept.shape[0], img_kept.shape[1] - LANES
    frame_rows, groups = 2 * rows, 2 * rows // TILE
    blocks = width // LANES + 1
    device = lax.axis_index("dev")
    odd, chip = lax.rem(device, 2), device // 2
    depth = chips.bit_length() - 1
    copies = [
        pltpu.make_async_copy(head, held, sems.at[i])
        for i, (head, held) in enumerate(((image_head, image_held), (text_head, text_held)))
    ]
    for copy in copies:
        copy.start()
    scale = jnp.exp(jnp.full((1, 1), log_scale[0], jnp.float32))
    bias = logit_bias[0]

    position = lax.broadcasted_iota(jnp.int32, (frame_rows, LANES), 0)
    lane = lax.broadcasted_iota(jnp.int32, (frame_rows, LANES), 1)
    from_mine = (position < rows) == (odd == 0)
    for apart in range(chips):
        target = jnp.bitwise_xor(chip, apart)
        mine, other = (far, far_other) if apart & 1 else (near, near_other)
        slot = sum(((apart >> level) & 1) << (depth - 1 - level) for level in range(1, depth))
        for block in range(blocks):
            columns = slice(block * LANES, (block + 1) * LANES)
            a, b = (frame_of(ref, slot, block, groups, lane) for ref in (mine, other))
            img_frames[target, :, columns] = jnp.where(from_mine, a, b).astype(jnp.bfloat16)
            txt_frames[target, :, columns] = jnp.where(from_mine, b, a).astype(jnp.bfloat16)
    flat = (chips * frame_rows, blocks * LANES)
    img_all, txt_all = img_frames[...].reshape(flat), txt_frames[...].reshape(flat)

    img_ids, txt_ids = img_all[:, width:], txt_all[:, width:]
    cosine = contract_last(img_all[:, :width], txt_all[:, :width])
    negative, decay, slopes = pair_terms(cosine, contract_last(img_ids, txt_ids), scale, bias)
    total = jnp.sum(jnp.maximum(negative, 0.0) + jnp.log1p(decay), keepdims=True)
    loss[0] = (total / pairs)[0, 0]
    grad_scale[0] = (scale * jnp.sum(slopes * cosine, keepdims=True) / pairs)[0, 0]
    grad_bias[0] = (jnp.sum(slopes, keepdims=True) / pairs)[0, 0]

    own_img, own_txt = (
        ref[chip, :, width:].astype(jnp.float32) for ref in (img_frames, txt_frames)
    )
    img_own_ids = jnp.where(odd == 0, own_img[:rows], own_img[rows:]).astype(jnp.bfloat16)
    txt_own_ids = jnp.where(odd == 0, own_txt[rows:], own_txt[:rows]).astype(jnp.bfloat16)
    sides = (
        (img_kept, img_own_ids, txt_all, txt_ids, copies[0], image_held, grad_images),
        (txt_kept, txt_own_ids, img_all, img_ids, copies[1], text_held, grad_texts),
    )
    for kept, own_ids, others, other_ids, copy, held, out in sides:
        unit, length = kept[:, :width], kept[:, width : width + 1]
        near = contract_last(unit.astype(jnp.bfloat16), others[:, :width])
        slopes = pair_terms(near, contract_last(own_ids, other_ids), scale, bias)[2]
        grad = scale * jnp.dot(
            slopes.astype(jnp.bfloat16), others[:, :width], preferred_element_type=jnp.float32
        )
        copy.wait()
        out[...] = backward_rows(grad, unit, length, held[...])


def on_device_small(
    image_feats, text_feats, image_head, text_head, log_scale, logit_bias, image_group, text_group
):
    devices = lax.axis_size("dev")
    chips = devices // 2
    rows, depth = image_feats.shape
    width = image_head.shape[1]
    blocks = width // LANES + 1
    tiles = 2 * rows // TILE * (width // LANES) + 1
    chunks = next(c for c in (3, 2, 1) if depth % (c * LANES) == 0 or c == 1)
    vmem, smem, hbm = (
        pl.BlockSpec(memory_space=pltpu.VMEM),
        pl.BlockSpec(memory_space=pltpu.SMEM),
        pl.BlockSpec(memory_space=pltpu.HBM),
    )
    f32, bf16 = jnp.float32, jnp.bfloat16
    payload, img_kept, txt_kept = pl.pallas_call(
        project_kernel,
        out_shape=(
            jax.ShapeDtypeStruct((tiles, TILE, LANES), bf16),
            jax.ShapeDtypeStruct((rows, width + LANES), f32),
            jax.ShapeDtypeStruct((rows, width + LANES), f32),
        ),
        in_specs=[hbm] * 6,
        out_specs=(vmem,) * 3,
        scratch_shapes=[
            pltpu.VMEM((depth, width), bf16),
            pltpu.VMEM((depth, width), bf16),
            pltpu.VMEM((2 * rows, width), f32),
            pltpu.VMEM((rows, depth), bf16),
            pltpu.VMEM((rows, depth), bf16),
            pltpu.SMEM((rows,), jnp.int32),
            pltpu.SMEM((rows,), jnp.int32),
            pltpu.SemaphoreType.DMA((2, chunks)),
            pltpu.SemaphoreType.DMA((4,)),
        ],
        compiler_params=pltpu.CompilerParams(vmem_limit_bytes=16 << 20),
        name="project",
    )(
        *(
            pltpu.with_memory_space_constraint(array, pltpu.HBM)
            for array in (image_group, text_group, image_feats, text_feats, image_head, text_head)
        )
    )

    def exchange(array, mask):
        return lax.ppermute(array, "dev", [(i, i ^ mask) for i in range(devices)])

    near = payload[None]
    mask = devices // 2
    while mask > 2:
        near = jnp.concatenate([near, exchange(near, mask)], axis=0)
        mask //= 2
    far = exchange(near, 2)
    near_other = exchange(near, 1)
    far_other = exchange(far, 1)

    loss, grad_images, grad_texts, grad_scale, grad_bias = pl.pallas_call(
        functools.partial(loss_kernel, chips, rows * devices),
        out_shape=(
            jax.ShapeDtypeStruct((1,), f32),
            jax.ShapeDtypeStruct((rows, depth), bf16),
            jax.ShapeDtypeStruct((rows, depth), bf16),
            jax.ShapeDtypeStruct((1,), f32),
            jax.ShapeDtypeStruct((1,), f32),
        ),
        in_specs=[smem, smem] + [vmem] * 6 + [hbm] * 2,
        out_specs=(smem, vmem, vmem, smem, smem),
        scratch_shapes=[pltpu.VMEM((chips, 2 * rows, blocks * LANES), bf16)] * 2
        + [pltpu.VMEM((depth, width), bf16)] * 2
        + [pltpu.SemaphoreType.DMA((2,))],
        compiler_params=pltpu.CompilerParams(vmem_limit_bytes=24 << 20),
        name="loss",
    )(
        log_scale.reshape(1),
        logit_bias.reshape(1),
        *(
            pltpu.with_memory_space_constraint(array, pltpu.VMEM)
            for array in (near, far, near_other, far_other, img_kept, txt_kept)
        ),
        *(pltpu.with_memory_space_constraint(head, pltpu.HBM) for head in (image_head, text_head)),
    )
    return (loss[0], grad_images, grad_texts, grad_scale[0], grad_bias[0])


def on_device(image_feats, text_feats, image_head, *rest):
    devices = lax.axis_size("dev")
    pairs = image_feats.shape[0] * devices
    small = (
        4 * pairs * pairs <= LOGIT_BUDGET
        and devices >= 4
        and devices & (devices - 1) == 0
        and image_head.shape[1] % LANES == 0
        and 2 * image_feats.shape[0] % TILE == 0
        and 2 * image_feats.shape[0] // TILE * BITS <= LANES
    )
    body = on_device_small if small else on_device_large
    return body(image_feats, text_feats, image_head, *rest)


def solution(mesh):
    placed = (P("dev", None), P("dev", None), P(), P(), P(), P(), P("dev"), P("dev"))
    return jax.shard_map(
        on_device,
        mesh=mesh,
        in_specs=placed,
        out_specs=(P(), P("dev", None), P("dev", None), P(), P()),
        check_vma=False,
    )
```

```python
import functools

import jax
import jax.numpy as jnp
from jax import lax
from jax.experimental import pallas as pl
from jax.experimental.pallas import tpu as pltpu
from jax.sharding import PartitionSpec as P

epsilon = 1e-06
LANES = 128
TILE = 8
BITS = 32
LOGIT_BUDGET = 4 << 20


def normalize(projected):
    length = jnp.sqrt(jnp.sum(projected * projected, axis=1, keepdims=True) + epsilon)
    return (projected / length, length)


def contract_last(a, b):
    return lax.dot_general(a, b, (((1,), (1,)), ((), ())), preferred_element_type=jnp.float32)


def backward_rows(grad_unit, unit_vec, length, weights):
    inner = jnp.sum(unit_vec * grad_unit, axis=1, keepdims=True)
    grad_proj = ((grad_unit - unit_vec * inner) / length).astype(jnp.bfloat16)
    return contract_last(grad_proj, weights).astype(jnp.bfloat16)


def on_device_large(
    image_feats, text_feats, image_head, text_head, log_scale, logit_bias, image_group, text_group
):
    img_unit, img_length = normalize(
        jnp.dot(image_feats, image_head, preferred_element_type=jnp.float32)
    )
    txt_unit, txt_length = normalize(
        jnp.dot(text_feats, text_head, preferred_element_type=jnp.float32)
    )
    img_emb = img_unit.astype(jnp.bfloat16)
    txt_emb = txt_unit.astype(jnp.bfloat16)
    logit_scale = jnp.exp(log_scale)
    pairs = image_feats.shape[0] * lax.axis_size("dev")
    emb_piece = lax.all_gather(jnp.stack([img_emb, txt_emb]), "dev", axis=1, tiled=True)
    id_piece = lax.all_gather(jnp.stack([image_group, text_group]), "dev", axis=1, tiled=True)

    def side(emb, others, group, other_group):
        cosine = contract_last(emb, others)
        label = jnp.where(group[:, None] == other_group[None, :], 1.0, -1.0).astype(jnp.float32)
        margin = label * (logit_scale * cosine + logit_bias)
        slopes = -label * jax.nn.sigmoid(-margin)
        grad = logit_scale * jnp.dot(
            slopes.astype(jnp.bfloat16), others, preferred_element_type=jnp.float32
        )
        return cosine, margin, slopes, grad

    cosine, margin, slopes, grad_img = side(img_emb, emb_piece[1], image_group, id_piece[1])
    local_sums = jnp.stack(
        [jnp.sum(jax.nn.softplus(-margin)), jnp.sum(slopes * cosine), jnp.sum(slopes)]
    )
    grad_txt = side(txt_emb, emb_piece[0], text_group, id_piece[0])[3]
    totals = lax.psum(local_sums, "dev")
    return (
        totals[0] / pairs,
        backward_rows(grad_img, img_unit, img_length, image_head),
        backward_rows(grad_txt, txt_unit, txt_length, text_head),
        logit_scale * totals[1] / pairs,
        totals[2] / pairs,
    )


def project_kernel(
    image_ids, text_ids, image_feats, text_feats, image_head, text_head,
    payload, img_kept, txt_kept,
    image_kept, text_kept, frame, image_rows, text_rows, image_marks, text_marks, head_sems, sems,
):
    rows, width = image_feats.shape[0], image_head.shape[1]
    depth, chunks = image_head.shape[0], head_sems.shape[1]
    step = depth // chunks
    odd = lax.rem(lax.axis_index("dev"), 2) == 1
    small = [
        pltpu.make_async_copy(source, target, sems.at[i])
        for i, (source, target) in enumerate(
            (
                (image_feats, image_rows),
                (text_feats, text_rows),
                (image_ids, image_marks),
                (text_ids, text_marks),
            )
        )
    ]
    large = [
        [
            pltpu.make_async_copy(
                head.at[pl.ds(i * step, step)], kept.at[pl.ds(i * step, step)], head_sems.at[side, i]
            )
            for i in range(chunks)
        ]
        for side, (head, kept) in enumerate(((image_head, image_kept), (text_head, text_kept)))
    ]
    small[0].start()
    for copy in large[0]:
        copy.start()
    for copy in small[1:]:
        copy.start()
    for copy in large[1]:
        copy.start()

    units = []
    sides = (
        (image_rows, image_kept, img_kept),
        (text_rows, text_kept, txt_kept),
    )
    for side, (feats, kept, out) in enumerate(sides):
        small[side].wait()
        projected = jnp.zeros((rows, width), jnp.float32)
        for i, copy in enumerate(large[side]):
            copy.wait()
            part = slice(i * step, (i + 1) * step)
            projected += jnp.dot(feats[:, part], kept[part], preferred_element_type=jnp.float32)
        unit, length = normalize(projected)
        out[:, :width] = unit
        out[:, width:] = jnp.broadcast_to(length, (rows, LANES))
        units.append(unit)
    frame[:rows] = jnp.where(odd, units[1], units[0])
    frame[rows:] = jnp.where(odd, units[0], units[1])
    groups = 2 * rows // TILE
    for block in range(width // LANES):
        columns = slice(block * LANES, (block + 1) * LANES)
        for group in range(groups):
            part = frame[group * TILE : (group + 1) * TILE, columns]
            payload[block * groups + group] = part.astype(jnp.bfloat16)

    small[2].wait()
    small[3].wait()
    position = lax.broadcasted_iota(jnp.int32, (TILE, LANES), 0)
    lane = lax.broadcasted_iota(jnp.int32, (TILE, LANES), 1)
    position += TILE * (lane // BITS)
    ids = jnp.zeros((TILE, LANES), jnp.int32)
    for row in range(rows):
        image_id, text_id = image_marks[row], text_marks[row]
        ids = jnp.where(position == row, jnp.where(odd, text_id, image_id), ids)
        ids = jnp.where(position == rows + row, jnp.where(odd, image_id, text_id), ids)
    bits = lax.shift_right_logical(ids, lane & (BITS - 1)) & 1
    payload[payload.shape[0] - 1] = jnp.where(bits == 1, 1.0, -1.0).astype(jnp.bfloat16)


def hop_orders(devices):
    bits = [1 << level for level in reversed(range(1, devices.bit_length() - 1))]
    first, rest = bits[:1], bits[1:]
    return first + rest, first + rest[1:] + rest[:1]


def parity(number, bits):
    return sum((number >> level) & 1 for level in range(bits)) % 2


def slot_of(apart, order):
    hops = [int(apart & bit != 0) for bit in order]
    return hops[-1] + 2 * sum(hop << level for level, hop in enumerate(hops[:-1]))


def frame_of(ref, slot, block, groups, lane):
    if (block + 1) * groups < ref.shape[1]:
        tiles = ref[slot, block * groups : (block + 1) * groups].astype(jnp.float32)
        return tiles.reshape(groups * TILE, LANES)
    packed = ref[slot, ref.shape[1] - 1].astype(jnp.float32)
    turned = [packed] + [
        pltpu.roll(packed, LANES - group * BITS, axis=1) for group in range(1, groups)
    ]
    return jnp.where(lane < BITS, jnp.concatenate(turned, axis=0), 0.0)


def pair_terms(cosine, matches, scale, bias):
    label = jnp.where(matches > BITS - 1.0, 1.0, -1.0)
    negative = -label * (scale * cosine + bias)
    decay = jnp.exp(-jnp.abs(negative))
    inverse = 1.0 / (1.0 + decay)
    slopes = -label * jnp.where(negative >= 0.0, inverse, decay * inverse)
    return negative, decay, slopes


def loss_kernel(
    chips, pairs, orders,
    log_scale, logit_bias, near, far, near_other, far_other, img_kept, txt_kept,
    image_head, text_head,
    loss, grad_images, grad_texts, grad_scale, grad_bias,
    img_frames, txt_frames, image_held, text_held, sems,
):
    rows, width = img_kept.shape[0], img_kept.shape[1] - LANES
    frame_rows, groups = 2 * rows, 2 * rows // TILE
    blocks = width // LANES + 1
    device = lax.axis_index("dev")
    odd, chip = lax.rem(device, 2), device // 2
    depth = chips.bit_length() - 1
    copies = [
        pltpu.make_async_copy(head, held, sems.at[i])
        for i, (head, held) in enumerate(((image_head, image_held), (text_head, text_held)))
    ]
    for copy in copies:
        copy.start()
    scale = jnp.exp(jnp.full((1, 1), log_scale[0], jnp.float32))
    bias = logit_bias[0]

    position = lax.broadcasted_iota(jnp.int32, (frame_rows, LANES), 0)
    lane = lax.broadcasted_iota(jnp.int32, (frame_rows, LANES), 1)
    from_mine = (position < rows) == (odd == 0)

    def assemble(held, passed):
        for apart in range(chips):
            target = jnp.bitwise_xor(chip, apart)
            flip = apart.bit_count() % 2 == 1
            (mine, slot), (other, other_slot) = (
                ((pieces[1] if slot % 2 else pieces[0]), slot // 2)
                for pieces, slot in (
                    ((near, far), slot_of(2 * apart, held)),
                    ((near_other, far_other), slot_of(2 * apart, passed)),
                )
            )
            for block in range(blocks):
                columns = slice(block * LANES, (block + 1) * LANES)
                a = frame_of(mine, slot, block, groups, lane)
                b = frame_of(other, other_slot, block, groups, lane)
                a, b = (b, a) if flip else (a, b)
                img_frames[target, :, columns] = jnp.where(from_mine, a, b).astype(jnp.bfloat16)
                txt_frames[target, :, columns] = jnp.where(from_mine, b, a).astype(jnp.bfloat16)

    kind = parity(device, depth + 1)
    pl.when(kind == 0)(functools.partial(assemble, orders[0], orders[1]))
    pl.when(kind == 1)(functools.partial(assemble, orders[1], orders[0]))
    flat = (chips * frame_rows, blocks * LANES)
    img_all, txt_all = img_frames[...].reshape(flat), txt_frames[...].reshape(flat)

    img_ids, txt_ids = img_all[:, width:], txt_all[:, width:]
    cosine = contract_last(img_all[:, :width], txt_all[:, :width])
    negative, decay, slopes = pair_terms(cosine, contract_last(img_ids, txt_ids), scale, bias)
    total = jnp.sum(jnp.maximum(negative, 0.0) + jnp.log1p(decay), keepdims=True)
    loss[0] = (total / pairs)[0, 0]
    grad_scale[0] = (scale * jnp.sum(slopes * cosine, keepdims=True) / pairs)[0, 0]
    grad_bias[0] = (jnp.sum(slopes, keepdims=True) / pairs)[0, 0]

    own_img, own_txt = (
        ref[chip, :, width:].astype(jnp.float32) for ref in (img_frames, txt_frames)
    )
    img_own_ids = jnp.where(odd == 0, own_img[:rows], own_img[rows:]).astype(jnp.bfloat16)
    txt_own_ids = jnp.where(odd == 0, own_txt[rows:], own_txt[:rows]).astype(jnp.bfloat16)
    sides = (
        (img_kept, img_own_ids, txt_all, txt_ids, copies[0], image_held, grad_images),
        (txt_kept, txt_own_ids, img_all, img_ids, copies[1], text_held, grad_texts),
    )
    for kept, own_ids, others, other_ids, copy, held, out in sides:
        unit, length = kept[:, :width], kept[:, width : width + 1]
        near = contract_last(unit.astype(jnp.bfloat16), others[:, :width])
        slopes = pair_terms(near, contract_last(own_ids, other_ids), scale, bias)[2]
        grad = scale * jnp.dot(
            slopes.astype(jnp.bfloat16), others[:, :width], preferred_element_type=jnp.float32
        )
        copy.wait()
        out[...] = backward_rows(grad, unit, length, held[...])


def on_device_small(
    image_feats, text_feats, image_head, text_head, log_scale, logit_bias, image_group, text_group
):
    devices = lax.axis_size("dev")
    chips = devices // 2
    rows, depth = image_feats.shape
    width = image_head.shape[1]
    blocks = width // LANES + 1
    tiles = 2 * rows // TILE * (width // LANES) + 1
    chunks = next(c for c in (3, 2, 1) if depth % (c * LANES) == 0 or c == 1)
    vmem, smem, hbm = (
        pl.BlockSpec(memory_space=pltpu.VMEM),
        pl.BlockSpec(memory_space=pltpu.SMEM),
        pl.BlockSpec(memory_space=pltpu.HBM),
    )
    f32, bf16 = jnp.float32, jnp.bfloat16
    payload, img_kept, txt_kept = pl.pallas_call(
        project_kernel,
        out_shape=(
            jax.ShapeDtypeStruct((tiles, TILE, LANES), bf16),
            jax.ShapeDtypeStruct((rows, width + LANES), f32),
            jax.ShapeDtypeStruct((rows, width + LANES), f32),
        ),
        in_specs=[hbm] * 6,
        out_specs=(vmem,) * 3,
        scratch_shapes=[
            pltpu.VMEM((depth, width), bf16),
            pltpu.VMEM((depth, width), bf16),
            pltpu.VMEM((2 * rows, width), f32),
            pltpu.VMEM((rows, depth), bf16),
            pltpu.VMEM((rows, depth), bf16),
            pltpu.SMEM((rows,), jnp.int32),
            pltpu.SMEM((rows,), jnp.int32),
            pltpu.SemaphoreType.DMA((2, chunks)),
            pltpu.SemaphoreType.DMA((4,)),
        ],
        compiler_params=pltpu.CompilerParams(vmem_limit_bytes=16 << 20),
        name="project",
    )(
        *(
            pltpu.with_memory_space_constraint(array, pltpu.HBM)
            for array in (image_group, text_group, image_feats, text_feats, image_head, text_head)
        )
    )

    orders = hop_orders(devices)
    bits = devices.bit_length() - 1

    def swap(array):
        return lax.ppermute(array, "dev", [(i, i ^ 1) for i in range(devices)])

    def hop(array, level):
        pairs = [(i, i ^ orders[parity(i, bits)][level] ^ 1) for i in range(devices)]
        return lax.ppermute(array, "dev", pairs)

    near = payload[None]
    for level in range(bits - 2):
        near = jnp.concatenate([near, hop(near, level)], axis=0)
    far = hop(near, bits - 2)
    near_other = swap(near)
    far_other = swap(far)

    loss, grad_images, grad_texts, grad_scale, grad_bias = pl.pallas_call(
        functools.partial(loss_kernel, chips, rows * devices, orders),
        out_shape=(
            jax.ShapeDtypeStruct((1,), f32),
            jax.ShapeDtypeStruct((rows, depth), bf16),
            jax.ShapeDtypeStruct((rows, depth), bf16),
            jax.ShapeDtypeStruct((1,), f32),
            jax.ShapeDtypeStruct((1,), f32),
        ),
        in_specs=[smem, smem] + [vmem] * 6 + [hbm] * 2,
        out_specs=(smem, vmem, vmem, smem, smem),
        scratch_shapes=[pltpu.VMEM((chips, 2 * rows, blocks * LANES), bf16)] * 2
        + [pltpu.VMEM((depth, width), bf16)] * 2
        + [pltpu.SemaphoreType.DMA((2,))],
        compiler_params=pltpu.CompilerParams(vmem_limit_bytes=24 << 20),
        name="loss",
    )(
        log_scale.reshape(1),
        logit_bias.reshape(1),
        *(
            pltpu.with_memory_space_constraint(array, pltpu.VMEM)
            for array in (near, far, near_other, far_other, img_kept, txt_kept)
        ),
        *(pltpu.with_memory_space_constraint(head, pltpu.HBM) for head in (image_head, text_head)),
    )
    return (loss[0], grad_images, grad_texts, grad_scale[0], grad_bias[0])


def on_device(image_feats, text_feats, image_head, *rest):
    devices = lax.axis_size("dev")
    pairs = image_feats.shape[0] * devices
    small = (
        4 * pairs * pairs <= LOGIT_BUDGET
        and devices >= 4
        and devices & (devices - 1) == 0
        and image_head.shape[1] % LANES == 0
        and 2 * image_feats.shape[0] % TILE == 0
        and 2 * image_feats.shape[0] // TILE * BITS <= LANES
    )
    body = on_device_small if small else on_device_large
    return body(image_feats, text_feats, image_head, *rest)


def solution(mesh):
    placed = (P("dev", None), P("dev", None), P(), P(), P(), P(), P("dev"), P("dev"))
    return jax.shard_map(
        on_device,
        mesh=mesh,
        in_specs=placed,
        out_specs=(P(), P("dev", None), P("dev", None), P(), P()),
        check_vma=False,
    )
```

```python
import functools

import jax
import jax.numpy as jnp
from jax import lax
from jax.experimental import pallas as pl
from jax.experimental.pallas import tpu as pltpu
from jax.sharding import PartitionSpec as P

epsilon = 1e-06
LANES = 128
TILE = 8
BITS = 32
LOGIT_BUDGET = 4 << 20
FETCH_FLOPS = 1 << 26


def normalize(projected):
    length = jnp.sqrt(jnp.sum(projected * projected, axis=1, keepdims=True) + epsilon)
    return (projected / length, length)


def contract_last(a, b):
    return lax.dot_general(a, b, (((1,), (1,)), ((), ())), preferred_element_type=jnp.float32)


def backward_rows(grad_unit, unit_vec, length, weights):
    inner = jnp.sum(unit_vec * grad_unit, axis=1, keepdims=True)
    grad_proj = ((grad_unit - unit_vec * inner) / length).astype(jnp.bfloat16)
    return contract_last(grad_proj, weights).astype(jnp.bfloat16)


def on_device_large(
    image_feats, text_feats, image_head, text_head, log_scale, logit_bias, image_group, text_group
):
    img_unit, img_length = normalize(
        jnp.dot(image_feats, image_head, preferred_element_type=jnp.float32)
    )
    txt_unit, txt_length = normalize(
        jnp.dot(text_feats, text_head, preferred_element_type=jnp.float32)
    )
    img_emb = img_unit.astype(jnp.bfloat16)
    txt_emb = txt_unit.astype(jnp.bfloat16)
    logit_scale = jnp.exp(log_scale)
    pairs = image_feats.shape[0] * lax.axis_size("dev")
    emb_piece = lax.all_gather(jnp.stack([img_emb, txt_emb]), "dev", axis=1, tiled=True)
    id_piece = lax.all_gather(jnp.stack([image_group, text_group]), "dev", axis=1, tiled=True)

    def side(emb, others, group, other_group):
        cosine = contract_last(emb, others)
        label = jnp.where(group[:, None] == other_group[None, :], 1.0, -1.0).astype(jnp.float32)
        margin = label * (logit_scale * cosine + logit_bias)
        slopes = -label * jax.nn.sigmoid(-margin)
        grad = logit_scale * jnp.dot(
            slopes.astype(jnp.bfloat16), others, preferred_element_type=jnp.float32
        )
        return cosine, margin, slopes, grad

    cosine, margin, slopes, grad_img = side(img_emb, emb_piece[1], image_group, id_piece[1])
    local_sums = jnp.stack(
        [jnp.sum(jax.nn.softplus(-margin)), jnp.sum(slopes * cosine), jnp.sum(slopes)]
    )
    grad_txt = side(txt_emb, emb_piece[0], text_group, id_piece[0])[3]
    totals = lax.psum(local_sums, "dev")
    return (
        totals[0] / pairs,
        backward_rows(grad_img, img_unit, img_length, image_head),
        backward_rows(grad_txt, txt_unit, txt_length, text_head),
        logit_scale * totals[1] / pairs,
        totals[2] / pairs,
    )


def project_kernel(
    image_ids, text_ids, image_feats, text_feats, image_head, text_head,
    payload, img_kept, txt_kept,
    image_kept, text_kept, frame, image_rows, text_rows,
    image_marks, text_marks, head_sems, sems,
):
    rows, width = image_feats.shape[0], image_head.shape[1]
    depth, chunks = image_head.shape[0], head_sems.shape[1]
    step = depth // chunks
    odd = lax.rem(lax.axis_index("dev"), 2) == 1
    small = [
        pltpu.make_async_copy(source, target, sems.at[i])
        for i, (source, target) in enumerate(
            (
                (image_feats, image_rows),
                (text_feats, text_rows),
                (image_ids, image_marks),
                (text_ids, text_marks),
            )
        )
    ]
    large = [
        [
            pltpu.make_async_copy(
                head.at[pl.ds(i * step, step)], kept.at[pl.ds(i * step, step)], head_sems.at[side, i]
            )
            for i in range(chunks)
        ]
        for side, (head, kept) in enumerate(((image_head, image_kept), (text_head, text_kept)))
    ]
    small[0].start()
    for copy in large[0]:
        copy.start()
    for copy in small[1:]:
        copy.start()
    for copy in large[1]:
        copy.start()

    units = []
    sides = (
        (image_rows, image_kept, img_kept),
        (text_rows, text_kept, txt_kept),
    )
    for side, (feats, kept, out) in enumerate(sides):
        small[side].wait()
        projected = jnp.zeros((rows, width), jnp.float32)
        for i, copy in enumerate(large[side]):
            copy.wait()
            part = slice(i * step, (i + 1) * step)
            projected += jnp.dot(feats[:, part], kept[part], preferred_element_type=jnp.float32)
        unit, length = normalize(projected)
        out[:, :width] = unit
        out[:, width:] = jnp.broadcast_to(length, (rows, LANES))
        units.append(unit)
    frame[:rows] = jnp.where(odd, units[1], units[0])
    frame[rows:] = jnp.where(odd, units[0], units[1])
    groups = 2 * rows // TILE
    for block in range(width // LANES):
        columns = slice(block * LANES, (block + 1) * LANES)
        for group in range(groups):
            part = frame[group * TILE : (group + 1) * TILE, columns]
            payload[block * groups + group] = part.astype(jnp.bfloat16)

    for copy in small[2:]:
        copy.wait()
    position = lax.broadcasted_iota(jnp.int32, (TILE, LANES), 0)
    lane = lax.broadcasted_iota(jnp.int32, (TILE, LANES), 1)
    position += TILE * (lane // BITS)
    ids = jnp.zeros((TILE, LANES), jnp.int32)
    for row in range(rows):
        image_id, text_id = image_marks[row], text_marks[row]
        ids = jnp.where(position == row, jnp.where(odd, text_id, image_id), ids)
        ids = jnp.where(position == rows + row, jnp.where(odd, image_id, text_id), ids)
    bits = lax.shift_right_logical(ids, lane & (BITS - 1)) & 1
    payload[payload.shape[0] - 1] = jnp.where(bits == 1, 1.0, -1.0).astype(jnp.bfloat16)


def hop_orders(devices):
    bits = [1 << level for level in reversed(range(1, devices.bit_length() - 1))]
    first, rest = bits[:1], bits[1:]
    return first + rest, first + rest[1:] + rest[:1]


def parity(number, bits):
    return sum((number >> level) & 1 for level in range(bits)) % 2


def slot_of(apart, order):
    hops = [int(apart & bit != 0) for bit in order]
    return hops[-1] + 2 * sum(hop << level for level, hop in enumerate(hops[:-1]))


def frame_of(ref, slot, block, groups, lane):
    if (block + 1) * groups < ref.shape[1]:
        tiles = ref[slot, block * groups : (block + 1) * groups].astype(jnp.float32)
        return tiles.reshape(groups * TILE, LANES)
    packed = ref[slot, ref.shape[1] - 1].astype(jnp.float32)
    turned = [packed] + [
        pltpu.roll(packed, LANES - group * BITS, axis=1) for group in range(1, groups)
    ]
    return jnp.where(lane < BITS, jnp.concatenate(turned, axis=0), 0.0)


def pair_terms(cosine, matches, scale, bias):
    label = jnp.where(matches > BITS - 1.0, 1.0, -1.0)
    negative = -label * (scale * cosine + bias)
    decay = jnp.exp(-jnp.abs(negative))
    inverse = 1.0 / (1.0 + decay)
    slopes = -label * jnp.where(negative >= 0.0, inverse, decay * inverse)
    return negative, decay, slopes


def loss_kernel(
    chips, pairs, orders,
    near, far, near_other, far_other, img_kept, txt_kept,
    image_head, text_head, scalars,
    loss, grad_images, grad_texts, grad_scale, grad_bias,
    img_frames, txt_frames, cosines, matches, image_out, text_out, sems,
):
    rows, width = img_kept.shape[0], img_kept.shape[1] - LANES
    frame_rows, groups = 2 * rows, 2 * rows // TILE
    blocks = width // LANES + 1
    device = lax.axis_index("dev")
    odd, chip = lax.rem(device, 2), device // 2
    depth = chips.bit_length() - 1
    scale, bias = scalars[0, :1, :1], scalars[1, :1, :1]

    position = lax.broadcasted_iota(jnp.int32, (frame_rows, LANES), 0)
    lane = lax.broadcasted_iota(jnp.int32, (frame_rows, LANES), 1)
    from_mine = (position < rows) == (odd == 0)

    def assemble(held, passed):
        for apart in range(chips):
            target = jnp.bitwise_xor(chip, apart)
            flip = apart.bit_count() % 2 == 1
            (mine, slot), (other, other_slot) = (
                ((pieces[1] if slot % 2 else pieces[0]), slot // 2)
                for pieces, slot in (
                    ((near, far), slot_of(2 * apart, held)),
                    ((near_other, far_other), slot_of(2 * apart, passed)),
                )
            )
            for block in range(blocks):
                columns = slice(block * LANES, (block + 1) * LANES)
                a = frame_of(mine, slot, block, groups, lane)
                b = frame_of(other, other_slot, block, groups, lane)
                a, b = (b, a) if flip else (a, b)
                img_frames[target, :, columns] = jnp.where(from_mine, a, b).astype(jnp.bfloat16)
                txt_frames[target, :, columns] = jnp.where(from_mine, b, a).astype(jnp.bfloat16)

    kind = parity(device, depth + 1)
    pl.when(kind == 0)(functools.partial(assemble, orders[0], orders[1]))
    pl.when(kind == 1)(functools.partial(assemble, orders[1], orders[0]))
    flat = (chips * frame_rows, blocks * LANES)
    img_all, txt_all = img_frames[...].reshape(flat), txt_frames[...].reshape(flat)

    img_emb, txt_emb = img_all[:, :width], txt_all[:, :width]
    img_ids, txt_ids = img_all[:, width:], txt_all[:, width:]
    cosines[...] = contract_last(img_emb, txt_emb)
    matches[...] = contract_last(img_ids, txt_ids)

    def own_rows(rows_of_chip, late):
        return jnp.where(late, rows_of_chip[rows:], rows_of_chip[:rows])

    here = pl.ds(pl.multiple_of(chip * frame_rows, TILE), frame_rows)
    own_txt_ids = own_rows(txt_frames[chip, :, width:].astype(jnp.float32), odd == 0)
    txt_unit = txt_kept[:, :width].astype(jnp.bfloat16)
    projected = []
    for kept, cosine, match, others in (
        (img_kept, own_rows(cosines[here], odd == 1), own_rows(matches[here], odd == 1), txt_emb),
        (
            txt_kept,
            contract_last(txt_unit, img_emb),
            contract_last(own_txt_ids.astype(jnp.bfloat16), img_ids),
            img_emb,
        ),
    ):
        unit, length = kept[:, :width], kept[:, width : width + 1]
        slopes = pair_terms(cosine, match, scale, bias)[2].astype(jnp.bfloat16)
        grad = scale * jnp.dot(slopes, others, preferred_element_type=jnp.float32)
        inner = jnp.sum(unit * grad, axis=1, keepdims=True)
        projected.append(((grad - unit * inner) / length).astype(jnp.bfloat16))

    def back(side, head, out, at=slice(None)):
        out[:, at] = contract_last(projected[side], head[at]).astype(jnp.bfloat16)

    def gather_sums(low, high, sums):
        for strip in range(low, high, TILE):
            strip_rows = slice(strip, strip + TILE)
            cosine = cosines[strip_rows]
            negative, decay, slopes = pair_terms(cosine, matches[strip_rows], scale, bias)
            terms = (jnp.maximum(negative, 0.0) + jnp.log1p(decay), slopes * cosine, slopes)
            sums = tuple(total + term for total, term in zip(sums, terms))
        return sums

    sums = (jnp.zeros((TILE, pairs), jnp.float32),) * 3
    back(0, image_head, image_out)
    back(1, text_head, text_out)
    sums = gather_sums(0, pairs, sums)
    copies = [
        pltpu.make_async_copy(image_out, grad_images, sems.at[0]),
        pltpu.make_async_copy(text_out, grad_texts, sems.at[1]),
    ]
    for copy in copies:
        copy.start()
    totals = [jnp.sum(total, keepdims=True) / pairs for total in sums]
    loss[0] = totals[0][0, 0]
    grad_scale[0] = (scale * totals[1])[0, 0]
    grad_bias[0] = totals[2][0, 0]
    for copy in copies:
        copy.wait()


def fetch_kernel(
    log_scale, logit_bias, image_head, text_head, near,
    image_held, text_held, scalars, sems,
):
    copies = [
        pltpu.make_async_copy(image_head, image_held, sems.at[0]),
        pltpu.make_async_copy(text_head, text_held, sems.at[1]),
    ]
    for copy in copies:
        copy.start()
    scalars[0] = jnp.exp(jnp.full((TILE, LANES), log_scale[0], jnp.float32))
    scalars[1] = jnp.full((TILE, LANES), logit_bias[0], jnp.float32)
    for copy in copies:
        copy.wait()


def on_device_small(
    image_feats, text_feats, image_head, text_head, log_scale, logit_bias, image_group, text_group
):
    devices = lax.axis_size("dev")
    chips = devices // 2
    rows, depth = image_feats.shape
    width = image_head.shape[1]
    blocks = width // LANES + 1
    tiles = 2 * rows // TILE * (width // LANES) + 1
    chunks = next(c for c in (1,) if depth % (c * LANES) == 0 or c == 1)
    vmem, smem, hbm = (
        pl.BlockSpec(memory_space=pltpu.VMEM),
        pl.BlockSpec(memory_space=pltpu.SMEM),
        pl.BlockSpec(memory_space=pltpu.HBM),
    )
    f32, bf16 = jnp.float32, jnp.bfloat16
    payload, img_kept, txt_kept = pl.pallas_call(
        project_kernel,
        out_shape=(
            jax.ShapeDtypeStruct((tiles, TILE, LANES), bf16),
            jax.ShapeDtypeStruct((rows, width + LANES), f32),
            jax.ShapeDtypeStruct((rows, width + LANES), f32),
        ),
        in_specs=[hbm] * 6,
        out_specs=(vmem,) * 3,
        scratch_shapes=[
            pltpu.VMEM((depth, width), bf16),
            pltpu.VMEM((depth, width), bf16),
            pltpu.VMEM((2 * rows, width), f32),
            pltpu.VMEM((rows, depth), bf16),
            pltpu.VMEM((rows, depth), bf16),
            pltpu.SMEM((rows,), jnp.int32),
            pltpu.SMEM((rows,), jnp.int32),
            pltpu.SemaphoreType.DMA((2, chunks)),
            pltpu.SemaphoreType.DMA((4,)),
        ],
        compiler_params=pltpu.CompilerParams(vmem_limit_bytes=16 << 20),
        name="project",
    )(
        *(
            pltpu.with_memory_space_constraint(array, pltpu.HBM)
            for array in (image_group, text_group, image_feats, text_feats, image_head, text_head)
        )
    )

    orders = hop_orders(devices)
    bits = devices.bit_length() - 1

    def swap(array):
        return lax.ppermute(array, "dev", [(i, i ^ 1) for i in range(devices)])

    def hop(array, level):
        pairs = [(i, i ^ orders[parity(i, bits)][level] ^ 1) for i in range(devices)]
        return lax.ppermute(array, "dev", pairs)

    near = payload[None]
    for level in range(bits - 2):
        near = jnp.concatenate([near, hop(near, level)], axis=0)
    far = hop(near, bits - 2)
    near_other = swap(near)
    image_held, text_held, scalars = pl.pallas_call(
        fetch_kernel,
        out_shape=(jax.ShapeDtypeStruct((depth, width), bf16),) * 2
        + (jax.ShapeDtypeStruct((2, TILE, LANES), f32),),
        in_specs=[smem, smem, hbm, hbm, pl.BlockSpec(memory_space=pl.ANY)],
        out_specs=(vmem,) * 3,
        scratch_shapes=[pltpu.SemaphoreType.DMA((2,))],
        cost_estimate=pl.CostEstimate(
            flops=FETCH_FLOPS, bytes_accessed=4 * depth * width, transcendentals=0
        ),
        compiler_params=pltpu.CompilerParams(vmem_limit_bytes=8 << 20),
        name="fetch",
    )(
        log_scale.reshape(1),
        logit_bias.reshape(1),
        pltpu.with_memory_space_constraint(image_head, pltpu.HBM),
        pltpu.with_memory_space_constraint(text_head, pltpu.HBM),
        near,
    )
    far, scalars = lax.optimization_barrier((far, scalars))
    far_other = swap(far)

    loss, grad_images, grad_texts, grad_scale, grad_bias = pl.pallas_call(
        functools.partial(loss_kernel, chips, rows * devices, orders),
        out_shape=(
            jax.ShapeDtypeStruct((1,), f32),
            jax.ShapeDtypeStruct((rows, depth), bf16),
            jax.ShapeDtypeStruct((rows, depth), bf16),
            jax.ShapeDtypeStruct((1,), f32),
            jax.ShapeDtypeStruct((1,), f32),
        ),
        in_specs=[vmem] * 9,
        out_specs=(smem, hbm, hbm, smem, smem),
        scratch_shapes=[pltpu.VMEM((chips, 2 * rows, blocks * LANES), bf16)] * 2
        + [pltpu.VMEM((rows * devices, rows * devices), f32)] * 2
        + [pltpu.VMEM((rows, depth), bf16)] * 2
        + [pltpu.SemaphoreType.DMA((2,))],
        compiler_params=pltpu.CompilerParams(vmem_limit_bytes=24 << 20),
        name="loss",
    )(
        *(
            pltpu.with_memory_space_constraint(array, pltpu.VMEM)
            for array in (near, far, near_other, far_other, img_kept, txt_kept)
            + (image_held, text_held, scalars)
        )
    )
    return (loss[0], grad_images, grad_texts, grad_scale[0], grad_bias[0])


def on_device(image_feats, text_feats, image_head, *rest):
    devices = lax.axis_size("dev")
    pairs = image_feats.shape[0] * devices
    small = (
        4 * pairs * pairs <= LOGIT_BUDGET
        and devices >= 4
        and devices & (devices - 1) == 0
        and image_head.shape[1] % LANES == 0
        and 2 * image_feats.shape[0] % TILE == 0
        and 2 * image_feats.shape[0] // TILE * BITS <= LANES
    )
    body = on_device_small if small else on_device_large
    return body(image_feats, text_feats, image_head, *rest)


def solution(mesh):
    placed = (P("dev", None), P("dev", None), P(), P(), P(), P(), P("dev"), P("dev"))
    return jax.shard_map(
        on_device,
        mesh=mesh,
        in_specs=placed,
        out_specs=(P(), P("dev", None), P("dev", None), P(), P()),
        check_vma=False,
    )
```

```python
import functools

import jax
import jax.numpy as jnp
from jax import lax
from jax.experimental import pallas as pl
from jax.experimental.pallas import tpu as pltpu
from jax.sharding import PartitionSpec as P

epsilon = 1e-06
LANES = 128
TILE = 8
BITS = 32
LOGIT_BUDGET = 4 << 20
FETCH_FLOPS = 1 << 26


def normalize(projected):
    length = jnp.sqrt(jnp.sum(projected * projected, axis=1, keepdims=True) + epsilon)
    return (projected / length, length)


def contract_last(a, b):
    return lax.dot_general(a, b, (((1,), (1,)), ((), ())), preferred_element_type=jnp.float32)


def backward_rows(grad_unit, unit_vec, length, weights):
    inner = jnp.sum(unit_vec * grad_unit, axis=1, keepdims=True)
    grad_proj = ((grad_unit - unit_vec * inner) / length).astype(jnp.bfloat16)
    return contract_last(grad_proj, weights).astype(jnp.bfloat16)


def on_device_large(
    image_feats, text_feats, image_head, text_head, log_scale, logit_bias, image_group, text_group
):
    img_unit, img_length = normalize(
        jnp.dot(image_feats, image_head, preferred_element_type=jnp.float32)
    )
    txt_unit, txt_length = normalize(
        jnp.dot(text_feats, text_head, preferred_element_type=jnp.float32)
    )
    img_emb = img_unit.astype(jnp.bfloat16)
    txt_emb = txt_unit.astype(jnp.bfloat16)
    logit_scale = jnp.exp(log_scale)
    pairs = image_feats.shape[0] * lax.axis_size("dev")
    emb_piece = lax.all_gather(jnp.stack([img_emb, txt_emb]), "dev", axis=1, tiled=True)
    id_piece = lax.all_gather(jnp.stack([image_group, text_group]), "dev", axis=1, tiled=True)

    def side(emb, others, group, other_group):
        cosine = contract_last(emb, others)
        label = jnp.where(group[:, None] == other_group[None, :], 1.0, -1.0).astype(jnp.float32)
        margin = label * (logit_scale * cosine + logit_bias)
        slopes = -label * jax.nn.sigmoid(-margin)
        grad = logit_scale * jnp.dot(
            slopes.astype(jnp.bfloat16), others, preferred_element_type=jnp.float32
        )
        return cosine, margin, slopes, grad

    cosine, margin, slopes, grad_img = side(img_emb, emb_piece[1], image_group, id_piece[1])
    local_sums = jnp.stack(
        [jnp.sum(jax.nn.softplus(-margin)), jnp.sum(slopes * cosine), jnp.sum(slopes)]
    )
    grad_txt = side(txt_emb, emb_piece[0], text_group, id_piece[0])[3]
    totals = lax.psum(local_sums, "dev")
    return (
        totals[0] / pairs,
        backward_rows(grad_img, img_unit, img_length, image_head),
        backward_rows(grad_txt, txt_unit, txt_length, text_head),
        logit_scale * totals[1] / pairs,
        totals[2] / pairs,
    )


def project_kernel(
    image_ids, text_ids, image_feats, text_feats, image_head, text_head,
    payload, img_kept, txt_kept,
    image_kept, text_kept, frame, image_rows, text_rows,
    image_marks, text_marks, head_sems, sems,
):
    rows, width = image_feats.shape[0], image_head.shape[1]
    depth, chunks = image_head.shape[0], head_sems.shape[1]
    step = depth // chunks
    odd = lax.rem(lax.axis_index("dev"), 2) == 1
    small = [
        pltpu.make_async_copy(source, target, sems.at[i])
        for i, (source, target) in enumerate(
            (
                (image_feats, image_rows),
                (text_feats, text_rows),
                (image_ids, image_marks),
                (text_ids, text_marks),
            )
        )
    ]
    large = [
        [
            pltpu.make_async_copy(
                head.at[pl.ds(i * step, step)], kept.at[pl.ds(i * step, step)], head_sems.at[side, i]
            )
            for i in range(chunks)
        ]
        for side, (head, kept) in enumerate(((image_head, image_kept), (text_head, text_kept)))
    ]
    small[0].start()
    for copy in large[0]:
        copy.start()
    for copy in small[1:]:
        copy.start()
    for copy in large[1]:
        copy.start()

    units = []
    sides = (
        (image_rows, image_kept, img_kept),
        (text_rows, text_kept, txt_kept),
    )
    for side, (feats, kept, out) in enumerate(sides):
        small[side].wait()
        projected = jnp.zeros((rows, width), jnp.float32)
        for i, copy in enumerate(large[side]):
            copy.wait()
            part = slice(i * step, (i + 1) * step)
            projected += jnp.dot(feats[:, part], kept[part], preferred_element_type=jnp.float32)
        unit, length = normalize(projected)
        out[:, :width] = unit
        out[:, width:] = jnp.broadcast_to(length, (rows, LANES))
        units.append(unit)
    frame[:rows] = jnp.where(odd, units[1], units[0])
    frame[rows:] = jnp.where(odd, units[0], units[1])
    groups = 2 * rows // TILE
    for block in range(width // LANES):
        columns = slice(block * LANES, (block + 1) * LANES)
        for group in range(groups):
            part = frame[group * TILE : (group + 1) * TILE, columns]
            payload[block * groups + group] = part.astype(jnp.bfloat16)

    for copy in small[2:]:
        copy.wait()
    position = lax.broadcasted_iota(jnp.int32, (TILE, LANES), 0)
    lane = lax.broadcasted_iota(jnp.int32, (TILE, LANES), 1)
    position += TILE * (lane // BITS)
    ids = jnp.zeros((TILE, LANES), jnp.int32)
    for row in range(rows):
        image_id, text_id = image_marks[row], text_marks[row]
        ids = jnp.where(position == row, jnp.where(odd, text_id, image_id), ids)
        ids = jnp.where(position == rows + row, jnp.where(odd, image_id, text_id), ids)
    bits = lax.shift_right_logical(ids, lane & (BITS - 1)) & 1
    payload[payload.shape[0] - 1] = jnp.where(bits == 1, 1.0, -1.0).astype(jnp.bfloat16)


def hop_orders(devices):
    bits = [1 << level for level in reversed(range(1, devices.bit_length() - 1))]
    first, rest = bits[:1], bits[1:]
    return first + rest, first + rest[1:] + rest[:1]


def parity(number, bits):
    return sum((number >> level) & 1 for level in range(bits)) % 2


def slot_of(apart, order):
    hops = [int(apart & bit != 0) for bit in order]
    return hops[-1] + 2 * sum(hop << level for level, hop in enumerate(hops[:-1]))


def frame_of(ref, slot, block, groups, lane):
    if (block + 1) * groups < ref.shape[1]:
        tiles = ref[slot, block * groups : (block + 1) * groups].astype(jnp.float32)
        return tiles.reshape(groups * TILE, LANES)
    packed = ref[slot, ref.shape[1] - 1].astype(jnp.float32)
    turned = [packed] + [
        pltpu.roll(packed, LANES - group * BITS, axis=1) for group in range(1, groups)
    ]
    return jnp.where(lane < BITS, jnp.concatenate(turned, axis=0), 0.0)


def pair_terms(cosine, matches, scale, bias):
    label = jnp.where(matches > BITS - 1.0, 1.0, -1.0)
    negative = -label * (scale * cosine + bias)
    decay = jnp.exp(-jnp.abs(negative))
    inverse = 1.0 / (1.0 + decay)
    slopes = -label * jnp.where(negative >= 0.0, inverse, decay * inverse)
    return negative, decay, slopes


def loss_kernel(
    chips, pairs, orders,
    near, far, near_other, far_other, img_kept, txt_kept,
    image_head, text_head, scalars,
    loss, grad_images, grad_texts, grad_scale, grad_bias,
    img_frames, txt_frames, cosines, matches, image_out, text_out,
    loss_out, scale_out, bias_out, sems,
):
    rows, width = img_kept.shape[0], img_kept.shape[1] - LANES
    frame_rows, groups = 2 * rows, 2 * rows // TILE
    blocks = width // LANES + 1
    device = lax.axis_index("dev")
    odd, chip = lax.rem(device, 2), device // 2
    depth = chips.bit_length() - 1
    scale, bias = scalars[0, :1, :1], scalars[1, :1, :1]

    position = lax.broadcasted_iota(jnp.int32, (frame_rows, LANES), 0)
    lane = lax.broadcasted_iota(jnp.int32, (frame_rows, LANES), 1)
    from_mine = (position < rows) == (odd == 0)

    def assemble(held, passed):
        for apart in range(chips):
            target = jnp.bitwise_xor(chip, apart)
            flip = apart.bit_count() % 2 == 1
            (mine, slot), (other, other_slot) = (
                ((pieces[1] if slot % 2 else pieces[0]), slot // 2)
                for pieces, slot in (
                    ((near, far), slot_of(2 * apart, held)),
                    ((near_other, far_other), slot_of(2 * apart, passed)),
                )
            )
            for block in range(blocks):
                columns = slice(block * LANES, (block + 1) * LANES)
                a = frame_of(mine, slot, block, groups, lane)
                b = frame_of(other, other_slot, block, groups, lane)
                a, b = (b, a) if flip else (a, b)
                img_frames[target, :, columns] = jnp.where(from_mine, a, b).astype(jnp.bfloat16)
                txt_frames[target, :, columns] = jnp.where(from_mine, b, a).astype(jnp.bfloat16)

    kind = parity(device, depth + 1)
    pl.when(kind == 0)(functools.partial(assemble, orders[0], orders[1]))
    pl.when(kind == 1)(functools.partial(assemble, orders[1], orders[0]))
    flat = (chips * frame_rows, blocks * LANES)
    img_all, txt_all = img_frames[...].reshape(flat), txt_frames[...].reshape(flat)

    img_emb, txt_emb = img_all[:, :width], txt_all[:, :width]
    img_ids, txt_ids = img_all[:, width:], txt_all[:, width:]
    cosines[...] = contract_last(img_emb, txt_emb)
    matches[...] = contract_last(img_ids, txt_ids)

    def own_rows(rows_of_chip, late):
        return jnp.where(late, rows_of_chip[rows:], rows_of_chip[:rows])

    here = pl.ds(pl.multiple_of(chip * frame_rows, TILE), frame_rows)
    own_txt_ids = own_rows(txt_frames[chip, :, width:].astype(jnp.float32), odd == 0)
    txt_unit = txt_kept[:, :width].astype(jnp.bfloat16)
    projected = []
    for kept, cosine, match, others in (
        (img_kept, own_rows(cosines[here], odd == 1), own_rows(matches[here], odd == 1), txt_emb),
        (
            txt_kept,
            contract_last(txt_unit, img_emb),
            contract_last(own_txt_ids.astype(jnp.bfloat16), img_ids),
            img_emb,
        ),
    ):
        unit, length = kept[:, :width], kept[:, width : width + 1]
        slopes = pair_terms(cosine, match, scale, bias)[2].astype(jnp.bfloat16)
        grad = scale * jnp.dot(slopes, others, preferred_element_type=jnp.float32)
        inner = jnp.sum(unit * grad, axis=1, keepdims=True)
        projected.append(((grad - unit * inner) / length).astype(jnp.bfloat16))

    def back(side, head, out, at=slice(None)):
        out[:, at] = contract_last(projected[side], head[at]).astype(jnp.bfloat16)

    def gather_sums(low, high, sums):
        for strip in range(low, high, TILE):
            strip_rows = slice(strip, strip + TILE)
            cosine = cosines[strip_rows]
            negative, decay, slopes = pair_terms(cosine, matches[strip_rows], scale, bias)
            terms = (jnp.maximum(negative, 0.0) + jnp.log1p(decay), slopes * cosine, slopes)
            sums = tuple(total + term for total, term in zip(sums, terms))
        return sums

    sums = (jnp.zeros((TILE, pairs), jnp.float32),) * 3
    copies = [
        pltpu.make_async_copy(image_out, grad_images, sems.at[0]),
        pltpu.make_async_copy(text_out, grad_texts, sems.at[1]),
        pltpu.make_async_copy(loss_out, loss, sems.at[2]),
        pltpu.make_async_copy(scale_out, grad_scale, sems.at[3]),
        pltpu.make_async_copy(bias_out, grad_bias, sems.at[4]),
    ]
    back(0, image_head, image_out)
    copies[0].start()
    back(1, text_head, text_out)
    copies[1].start()
    sums = gather_sums(0, pairs, sums)
    totals = [jnp.sum(total, keepdims=True) / pairs for total in sums]
    loss_out[0] = totals[0][0, 0]
    scale_out[0] = (scale * totals[1])[0, 0]
    bias_out[0] = totals[2][0, 0]
    for copy in copies[2:]:
        copy.start()
    for copy in copies:
        copy.wait()


def fetch_kernel(
    log_scale, logit_bias, image_head, text_head, near,
    image_held, text_held, scalars, sems,
):
    copies = [
        pltpu.make_async_copy(image_head, image_held, sems.at[0]),
        pltpu.make_async_copy(text_head, text_held, sems.at[1]),
    ]
    for copy in copies:
        copy.start()
    scalars[0] = jnp.exp(jnp.full((TILE, LANES), log_scale[0], jnp.float32))
    scalars[1] = jnp.full((TILE, LANES), logit_bias[0], jnp.float32)
    for copy in copies:
        copy.wait()


def on_device_small(
    image_feats, text_feats, image_head, text_head, log_scale, logit_bias, image_group, text_group
):
    devices = lax.axis_size("dev")
    chips = devices // 2
    rows, depth = image_feats.shape
    width = image_head.shape[1]
    blocks = width // LANES + 1
    tiles = 2 * rows // TILE * (width // LANES) + 1
    chunks = next(c for c in (1,) if depth % (c * LANES) == 0 or c == 1)
    vmem, smem, hbm = (
        pl.BlockSpec(memory_space=pltpu.VMEM),
        pl.BlockSpec(memory_space=pltpu.SMEM),
        pl.BlockSpec(memory_space=pltpu.HBM),
    )
    f32, bf16 = jnp.float32, jnp.bfloat16
    payload, img_kept, txt_kept = pl.pallas_call(
        project_kernel,
        out_shape=(
            jax.ShapeDtypeStruct((tiles, TILE, LANES), bf16),
            jax.ShapeDtypeStruct((rows, width + LANES), f32),
            jax.ShapeDtypeStruct((rows, width + LANES), f32),
        ),
        in_specs=[hbm] * 6,
        out_specs=(vmem,) * 3,
        scratch_shapes=[
            pltpu.VMEM((depth, width), bf16),
            pltpu.VMEM((depth, width), bf16),
            pltpu.VMEM((2 * rows, width), f32),
            pltpu.VMEM((rows, depth), bf16),
            pltpu.VMEM((rows, depth), bf16),
            pltpu.SMEM((rows,), jnp.int32),
            pltpu.SMEM((rows,), jnp.int32),
            pltpu.SemaphoreType.DMA((2, chunks)),
            pltpu.SemaphoreType.DMA((4,)),
        ],
        compiler_params=pltpu.CompilerParams(vmem_limit_bytes=16 << 20),
        name="project",
    )(
        *(
            pltpu.with_memory_space_constraint(array, pltpu.HBM)
            for array in (image_group, text_group, image_feats, text_feats, image_head, text_head)
        )
    )

    orders = hop_orders(devices)
    bits = devices.bit_length() - 1

    def swap(array):
        return lax.ppermute(array, "dev", [(i, i ^ 1) for i in range(devices)])

    def hop(array, level):
        pairs = [(i, i ^ orders[parity(i, bits)][level] ^ 1) for i in range(devices)]
        return lax.ppermute(array, "dev", pairs)

    near = payload[None]
    for level in range(bits - 2):
        near = jnp.concatenate([near, hop(near, level)], axis=0)
    far = hop(near, bits - 2)
    near_other = swap(near)
    image_held, text_held, scalars = pl.pallas_call(
        fetch_kernel,
        out_shape=(jax.ShapeDtypeStruct((depth, width), bf16),) * 2
        + (jax.ShapeDtypeStruct((2, TILE, LANES), f32),),
        in_specs=[smem, smem, hbm, hbm, pl.BlockSpec(memory_space=pl.ANY)],
        out_specs=(vmem,) * 3,
        scratch_shapes=[pltpu.SemaphoreType.DMA((2,))],
        cost_estimate=pl.CostEstimate(
            flops=FETCH_FLOPS, bytes_accessed=4 * depth * width, transcendentals=0
        ),
        compiler_params=pltpu.CompilerParams(vmem_limit_bytes=8 << 20),
        name="fetch",
    )(
        log_scale.reshape(1),
        logit_bias.reshape(1),
        pltpu.with_memory_space_constraint(image_head, pltpu.HBM),
        pltpu.with_memory_space_constraint(text_head, pltpu.HBM),
        near,
    )
    far, scalars = lax.optimization_barrier((far, scalars))
    far_other = swap(far)

    loss, grad_images, grad_texts, grad_scale, grad_bias = pl.pallas_call(
        functools.partial(loss_kernel, chips, rows * devices, orders),
        out_shape=(
            jax.ShapeDtypeStruct((1,), f32),
            jax.ShapeDtypeStruct((rows, depth), bf16),
            jax.ShapeDtypeStruct((rows, depth), bf16),
            jax.ShapeDtypeStruct((1,), f32),
            jax.ShapeDtypeStruct((1,), f32),
        ),
        in_specs=[vmem] * 9,
        out_specs=(hbm,) * 5,
        scratch_shapes=[pltpu.VMEM((chips, 2 * rows, blocks * LANES), bf16)] * 2
        + [pltpu.VMEM((rows * devices, rows * devices), f32)] * 2
        + [pltpu.VMEM((rows, depth), bf16)] * 2
        + [pltpu.SMEM((1,), f32)] * 3
        + [pltpu.SemaphoreType.DMA((5,))],
        compiler_params=pltpu.CompilerParams(vmem_limit_bytes=24 << 20),
        name="loss",
    )(
        *(
            pltpu.with_memory_space_constraint(array, pltpu.VMEM)
            for array in (near, far, near_other, far_other, img_kept, txt_kept)
            + (image_held, text_held, scalars)
        )
    )
    return (loss[0], grad_images, grad_texts, grad_scale[0], grad_bias[0])


def on_device(image_feats, text_feats, image_head, *rest):
    devices = lax.axis_size("dev")
    pairs = image_feats.shape[0] * devices
    small = (
        4 * pairs * pairs <= LOGIT_BUDGET
        and devices >= 4
        and devices & (devices - 1) == 0
        and image_head.shape[1] % LANES == 0
        and 2 * image_feats.shape[0] % TILE == 0
        and 2 * image_feats.shape[0] // TILE * BITS <= LANES
    )
    body = on_device_small if small else on_device_large
    return body(image_feats, text_feats, image_head, *rest)


def solution(mesh):
    placed = (P("dev", None), P("dev", None), P(), P(), P(), P(), P("dev"), P("dev"))
    return jax.shard_map(
        on_device,
        mesh=mesh,
        in_specs=placed,
        out_specs=(P(), P("dev", None), P("dev", None), P(), P()),
        check_vma=False,
    )
```

```python
import functools

import jax
import jax.numpy as jnp
from jax import lax
from jax.experimental import pallas as pl
from jax.experimental.pallas import tpu as pltpu
from jax.sharding import PartitionSpec as P


epsilon = 1e-06
LANES = 128
TILE = 8
BITS = 32
LOGIT_BUDGET = 4 << 20
SIDE_FLOPS = 1 << 26


def normalize(projected):
    length = jnp.sqrt(jnp.sum(projected * projected, axis=1, keepdims=True) + epsilon)
    return (projected / length, length)


def contract_last(a, b):
    return lax.dot_general(a, b, (((1,), (1,)), ((), ())), preferred_element_type=jnp.float32)


def backward_rows(grad_unit, unit_vec, length, weights):
    inner = jnp.sum(unit_vec * grad_unit, axis=1, keepdims=True)
    grad_proj = ((grad_unit - unit_vec * inner) / length).astype(jnp.bfloat16)
    return contract_last(grad_proj, weights).astype(jnp.bfloat16)


def on_device_large(
    image_feats, text_feats, image_head, text_head, log_scale, logit_bias, image_group, text_group
):
    img_unit, img_length = normalize(
        jnp.dot(image_feats, image_head, preferred_element_type=jnp.float32)
    )
    txt_unit, txt_length = normalize(
        jnp.dot(text_feats, text_head, preferred_element_type=jnp.float32)
    )
    img_emb = img_unit.astype(jnp.bfloat16)
    txt_emb = txt_unit.astype(jnp.bfloat16)
    logit_scale = jnp.exp(log_scale)
    pairs = image_feats.shape[0] * lax.axis_size("dev")
    emb_piece = lax.all_gather(jnp.stack([img_emb, txt_emb]), "dev", axis=1, tiled=True)
    id_piece = lax.all_gather(jnp.stack([image_group, text_group]), "dev", axis=1, tiled=True)

    def side(emb, others, group, other_group):
        cosine = contract_last(emb, others)
        label = jnp.where(group[:, None] == other_group[None, :], 1.0, -1.0).astype(jnp.float32)
        margin = label * (logit_scale * cosine + logit_bias)
        slopes = -label * jax.nn.sigmoid(-margin)
        grad = logit_scale * jnp.dot(
            slopes.astype(jnp.bfloat16), others, preferred_element_type=jnp.float32
        )
        return cosine, margin, slopes, grad

    cosine, margin, slopes, grad_img = side(img_emb, emb_piece[1], image_group, id_piece[1])
    local_sums = jnp.stack(
        [jnp.sum(jax.nn.softplus(-margin)), jnp.sum(slopes * cosine), jnp.sum(slopes)]
    )
    grad_txt = side(txt_emb, emb_piece[0], text_group, id_piece[0])[3]
    totals = lax.psum(local_sums, "dev")
    return (
        totals[0] / pairs,
        backward_rows(grad_img, img_unit, img_length, image_head),
        backward_rows(grad_txt, txt_unit, txt_length, text_head),
        logit_scale * totals[1] / pairs,
        totals[2] / pairs,
    )


def project_kernel(
    image_ids, text_ids, image_feats, text_feats, image_head, text_head,
    payload, img_kept, txt_kept,
    image_kept, text_kept, frame, image_rows, text_rows,
    image_marks, text_marks, head_sems, sems,
):
    rows, width = image_feats.shape[0], image_head.shape[1]
    depth, chunks = image_head.shape[0], head_sems.shape[1]
    step = depth // chunks
    odd = lax.rem(lax.axis_index("dev"), 2) == 1
    small = [
        pltpu.make_async_copy(source, target, sems.at[i])
        for i, (source, target) in enumerate(
            (
                (image_feats, image_rows),
                (text_feats, text_rows),
                (image_ids, image_marks),
                (text_ids, text_marks),
            )
        )
    ]
    large = [
        [
            pltpu.make_async_copy(
                head.at[pl.ds(i * step, step)], kept.at[pl.ds(i * step, step)], head_sems.at[side, i]
            )
            for i in range(chunks)
        ]
        for side, (head, kept) in enumerate(((image_head, image_kept), (text_head, text_kept)))
    ]
    small[0].start()
    for copy in large[0]:
        copy.start()
    for copy in small[1:]:
        copy.start()
    for copy in large[1]:
        copy.start()

    units = []
    sides = (
        (image_rows, image_kept, img_kept),
        (text_rows, text_kept, txt_kept),
    )
    for side, (feats, kept, out) in enumerate(sides):
        small[side].wait()
        projected = jnp.zeros((rows, width), jnp.float32)
        for i, copy in enumerate(large[side]):
            copy.wait()
            part = slice(i * step, (i + 1) * step)
            projected += jnp.dot(feats[:, part], kept[part], preferred_element_type=jnp.float32)
        unit, length = normalize(projected)
        out[:, :width] = unit
        out[:, width:] = jnp.broadcast_to(length, (rows, LANES))
        units.append(unit)
    frame[:rows] = jnp.where(odd, units[1], units[0])
    frame[rows:] = jnp.where(odd, units[0], units[1])
    groups = 2 * rows // TILE
    for block in range(width // LANES):
        columns = slice(block * LANES, (block + 1) * LANES)
        for group in range(groups):
            part = frame[group * TILE : (group + 1) * TILE, columns]
            payload[block * groups + group] = part.astype(jnp.bfloat16)

    for copy in small[2:]:
        copy.wait()
    position = lax.broadcasted_iota(jnp.int32, (TILE, LANES), 0)
    lane = lax.broadcasted_iota(jnp.int32, (TILE, LANES), 1)
    position += TILE * (lane // BITS)
    ids = jnp.zeros((TILE, LANES), jnp.int32)
    for row in range(rows):
        image_id, text_id = image_marks[row], text_marks[row]
        ids = jnp.where(position == row, jnp.where(odd, text_id, image_id), ids)
        ids = jnp.where(position == rows + row, jnp.where(odd, image_id, text_id), ids)
    bits = lax.shift_right_logical(ids, lane & (BITS - 1)) & 1
    payload[payload.shape[0] - 1] = jnp.where(bits == 1, 1.0, -1.0).astype(jnp.bfloat16)


def hop_orders(devices):
    bits = [1 << level for level in reversed(range(1, devices.bit_length() - 1))]
    first, rest = bits[:1], bits[1:]
    return first + rest, first + rest[1:] + rest[:1]


def parity(number, bits):
    return sum((number >> level) & 1 for level in range(bits)) % 2


def slot_of(apart, order):
    hops = [int(apart & bit != 0) for bit in order]
    return hops[-1] + 2 * hops[-2] + 4 * sum(hop << level for level, hop in enumerate(hops[:-2]))


def frame_of(ref, slot, block, groups, lane):
    if (block + 1) * groups < ref.shape[1]:
        tiles = ref[slot, block * groups : (block + 1) * groups].astype(jnp.float32)
        return tiles.reshape(groups * TILE, LANES)
    packed = ref[slot, ref.shape[1] - 1].astype(jnp.float32)
    turned = [packed] + [
        pltpu.roll(packed, LANES - group * BITS, axis=1) for group in range(1, groups)
    ]
    return jnp.where(lane < BITS, jnp.concatenate(turned, axis=0), 0.0)


def pair_terms(cosine, matches, scale, bias):
    label = jnp.where(matches > BITS - 1.0, 1.0, -1.0)
    negative = -label * (scale * cosine + bias)
    decay = jnp.exp(-jnp.abs(negative))
    inverse = 1.0 / (1.0 + decay)
    slopes = -label * jnp.where(negative >= 0.0, inverse, decay * inverse)
    return negative, decay, slopes


def loss_kernel(chips, pairs, orders, *refs):
    mine_pieces, other_pieces = refs[:4], refs[4:8]
    (
        img_kept, txt_kept, scalars, image_head, text_head,
        loss, grad_images, grad_texts, grad_scale, grad_bias,
        img_frames, txt_frames, cosines, matches, image_out, text_out,
        loss_out, scale_out, bias_out, sems,
    ) = refs[8:]
    rows, width = img_kept.shape[0], img_kept.shape[1] - LANES
    frame_rows, groups = 2 * rows, 2 * rows // TILE
    blocks = width // LANES + 1
    device = lax.axis_index("dev")
    odd, chip = lax.rem(device, 2), device // 2
    depth = chips.bit_length() - 1
    scale, bias = scalars[0, :1, :1], scalars[1, :1, :1]

    position = lax.broadcasted_iota(jnp.int32, (frame_rows, LANES), 0)
    lane = lax.broadcasted_iota(jnp.int32, (frame_rows, LANES), 1)
    from_mine = (position < rows) == (odd == 0)

    def assemble(held, passed):
        for apart in range(chips):
            target = jnp.bitwise_xor(chip, apart)
            flip = apart.bit_count() % 2 == 1
            (mine, slot), (other, other_slot) = (
                (pieces[slot % 4], slot // 4)
                for pieces, slot in (
                    (mine_pieces, slot_of(2 * apart, held)),
                    (other_pieces, slot_of(2 * apart, passed)),
                )
            )
            for block in range(blocks):
                columns = slice(block * LANES, (block + 1) * LANES)
                a = frame_of(mine, slot, block, groups, lane)
                b = frame_of(other, other_slot, block, groups, lane)
                a, b = (b, a) if flip else (a, b)
                img_frames[target, :, columns] = jnp.where(from_mine, a, b).astype(jnp.bfloat16)
                txt_frames[target, :, columns] = jnp.where(from_mine, b, a).astype(jnp.bfloat16)

    kind = parity(device, depth + 1)
    pl.when(kind == 0)(functools.partial(assemble, orders[0], orders[1]))
    pl.when(kind == 1)(functools.partial(assemble, orders[1], orders[0]))
    flat = (chips * frame_rows, blocks * LANES)
    img_all, txt_all = img_frames[...].reshape(flat), txt_frames[...].reshape(flat)

    img_emb, txt_emb = img_all[:, :width], txt_all[:, :width]
    img_ids, txt_ids = img_all[:, width:], txt_all[:, width:]
    cosines[...] = contract_last(img_emb, txt_emb)
    matches[...] = contract_last(img_ids, txt_ids)

    def own_rows(rows_of_chip, late):
        return jnp.where(late, rows_of_chip[rows:], rows_of_chip[:rows])

    here = pl.ds(pl.multiple_of(chip * frame_rows, TILE), frame_rows)
    own_txt_ids = own_rows(txt_frames[chip, :, width:].astype(jnp.float32), odd == 0)
    txt_unit = txt_kept[:, :width].astype(jnp.bfloat16)
    projected = []
    for kept, cosine, match, others in (
        (img_kept, own_rows(cosines[here], odd == 1), own_rows(matches[here], odd == 1), txt_emb),
        (
            txt_kept,
            contract_last(txt_unit, img_emb),
            contract_last(own_txt_ids.astype(jnp.bfloat16), img_ids),
            img_emb,
        ),
    ):
        unit, length = kept[:, :width], kept[:, width : width + 1]
        slopes = pair_terms(cosine, match, scale, bias)[2].astype(jnp.bfloat16)
        grad = scale * jnp.dot(slopes, others, preferred_element_type=jnp.float32)
        inner = jnp.sum(unit * grad, axis=1, keepdims=True)
        projected.append(((grad - unit * inner) / length).astype(jnp.bfloat16))

    def back(side, head, out, at=slice(None)):
        out[:, at] = contract_last(projected[side], head[at]).astype(jnp.bfloat16)

    def gather_sums(low, high, sums):
        for strip in range(low, high, TILE):
            strip_rows = slice(strip, strip + TILE)
            cosine = cosines[strip_rows]
            negative, decay, slopes = pair_terms(cosine, matches[strip_rows], scale, bias)
            terms = (jnp.maximum(negative, 0.0) + jnp.log1p(decay), slopes * cosine, slopes)
            sums = tuple(total + term for total, term in zip(sums, terms))
        return sums

    sums = (jnp.zeros((TILE, pairs), jnp.float32),) * 3
    copies = [
        pltpu.make_async_copy(image_out, grad_images, sems.at[0]),
        pltpu.make_async_copy(text_out, grad_texts, sems.at[1]),
        pltpu.make_async_copy(loss_out, loss, sems.at[2]),
        pltpu.make_async_copy(scale_out, grad_scale, sems.at[3]),
        pltpu.make_async_copy(bias_out, grad_bias, sems.at[4]),
    ]
    back(0, image_head, image_out)
    copies[0].start()
    back(1, text_head, text_out)
    copies[1].start()
    sums = gather_sums(0, pairs, sums)
    totals = [jnp.sum(total, keepdims=True) / pairs for total in sums]
    loss_out[0] = totals[0][0, 0]
    scale_out[0] = (scale * totals[1])[0, 0]
    bias_out[0] = totals[2][0, 0]
    for copy in copies[2:]:
        copy.start()
    for copy in copies:
        copy.wait()


def fetch_kernel(image_head, text_head, new, image_held, text_held, sems):
    copies = [
        pltpu.make_async_copy(image_head, image_held, sems.at[0]),
        pltpu.make_async_copy(text_head, text_held, sems.at[1]),
    ]
    for copy in copies:
        copy.start()
    for copy in copies:
        copy.wait()


def scalar_kernel(log_scale, logit_bias, payload, scalars):
    scalars[0] = jnp.exp(jnp.full(scalars.shape[1:], log_scale[0], jnp.float32))
    scalars[1] = jnp.full(scalars.shape[1:], logit_bias[0], jnp.float32)


def on_device_small(
    image_feats, text_feats, image_head, text_head, log_scale, logit_bias, image_group, text_group
):
    devices = lax.axis_size("dev")
    chips = devices // 2
    rows, depth = image_feats.shape
    width = image_head.shape[1]
    blocks = width // LANES + 1
    tiles = 2 * rows // TILE * (width // LANES) + 1
    chunks = next(c for c in (1,) if depth % (c * LANES) == 0 or c == 1)
    vmem, smem, hbm = (
        pl.BlockSpec(memory_space=pltpu.VMEM),
        pl.BlockSpec(memory_space=pltpu.SMEM),
        pl.BlockSpec(memory_space=pltpu.HBM),
    )
    f32, bf16 = jnp.float32, jnp.bfloat16
    payload, img_kept, txt_kept = pl.pallas_call(
        project_kernel,
        out_shape=(
            jax.ShapeDtypeStruct((tiles, TILE, LANES), bf16),
            jax.ShapeDtypeStruct((rows, width + LANES), f32),
            jax.ShapeDtypeStruct((rows, width + LANES), f32),
        ),
        in_specs=[hbm] * 6,
        out_specs=(vmem,) * 3,
        scratch_shapes=[
            pltpu.VMEM((depth, width), bf16),
            pltpu.VMEM((depth, width), bf16),
            pltpu.VMEM((2 * rows, width), f32),
            pltpu.VMEM((rows, depth), bf16),
            pltpu.VMEM((rows, depth), bf16),
            pltpu.SMEM((rows,), jnp.int32),
            pltpu.SMEM((rows,), jnp.int32),
            pltpu.SemaphoreType.DMA((2, chunks)),
            pltpu.SemaphoreType.DMA((4,)),
        ],
        compiler_params=pltpu.CompilerParams(vmem_limit_bytes=16 << 20),
        name="project",
    )(
        *(
            pltpu.with_memory_space_constraint(array, pltpu.HBM)
            for array in (image_group, text_group, image_feats, text_feats, image_head, text_head)
        )
    )

    orders = hop_orders(devices)
    bits = devices.bit_length() - 1

    def swap(array):
        return lax.ppermute(array, "dev", [(i, i ^ 1) for i in range(devices)])

    def hop(array, level):
        pairs = [(i, i ^ orders[parity(i, bits)][level] ^ 1) for i in range(devices)]
        return lax.ppermute(array, "dev", pairs)

    scalars = pl.pallas_call(
        scalar_kernel,
        out_shape=jax.ShapeDtypeStruct((2, TILE, LANES), f32),
        in_specs=[smem, smem, pl.BlockSpec(memory_space=pl.ANY)],
        out_specs=vmem,
        cost_estimate=pl.CostEstimate(flops=SIDE_FLOPS, bytes_accessed=64, transcendentals=0),
        compiler_params=pltpu.CompilerParams(vmem_limit_bytes=1 << 20),
        name="scalars",
    )(log_scale.reshape(1), logit_bias.reshape(1), payload)
    old = payload[None]
    for level in range(bits - 3):
        old = jnp.concatenate([old, hop(old, level)], axis=0)
        if level == 0:
            old, scalars = lax.optimization_barrier((old, scalars))
    new = hop(old, bits - 3)
    old_far = hop(old, bits - 2)
    new_far = hop(new, bits - 2)
    image_held, text_held = pl.pallas_call(
        fetch_kernel,
        out_shape=(jax.ShapeDtypeStruct((depth, width), bf16),) * 2,
        in_specs=[hbm, hbm, pl.BlockSpec(memory_space=pl.ANY)],
        out_specs=(vmem,) * 2,
        scratch_shapes=[pltpu.SemaphoreType.DMA((2,))],
        cost_estimate=pl.CostEstimate(
            flops=SIDE_FLOPS, bytes_accessed=4 * depth * width, transcendentals=0
        ),
        compiler_params=pltpu.CompilerParams(vmem_limit_bytes=8 << 20),
        name="fetch",
    )(
        pltpu.with_memory_space_constraint(image_head, pltpu.HBM),
        pltpu.with_memory_space_constraint(text_head, pltpu.HBM),
        new,
    )
    old_other = swap(old)
    new_other = swap(new)
    old_far_other = swap(old_far)
    new_far, image_held, text_held, old_other, new_other, old_far_other = lax.optimization_barrier(
        (new_far, image_held, text_held, old_other, new_other, old_far_other)
    )
    new_far_other = swap(new_far)
    pieces = (old, old_far, new, new_far, old_other, old_far_other, new_other, new_far_other)

    loss, grad_images, grad_texts, grad_scale, grad_bias = pl.pallas_call(
        functools.partial(loss_kernel, chips, rows * devices, orders),
        out_shape=(
            jax.ShapeDtypeStruct((1,), f32),
            jax.ShapeDtypeStruct((rows, depth), bf16),
            jax.ShapeDtypeStruct((rows, depth), bf16),
            jax.ShapeDtypeStruct((1,), f32),
            jax.ShapeDtypeStruct((1,), f32),
        ),
        in_specs=[vmem] * 13,
        out_specs=(hbm,) * 5,
        scratch_shapes=[pltpu.VMEM((chips, 2 * rows, blocks * LANES), bf16)] * 2
        + [pltpu.VMEM((rows * devices, rows * devices), f32)] * 2
        + [pltpu.VMEM((rows, depth), bf16)] * 2
        + [pltpu.SMEM((1,), f32)] * 3
        + [pltpu.SemaphoreType.DMA((5,))],
        compiler_params=pltpu.CompilerParams(vmem_limit_bytes=24 << 20),
        name="loss",
    )(
        *(
            pltpu.with_memory_space_constraint(array, pltpu.VMEM)
            for array in pieces
            + (img_kept, txt_kept, scalars, image_held, text_held)
        )
    )
    return (loss[0], grad_images, grad_texts, grad_scale[0], grad_bias[0])


def on_device(image_feats, text_feats, image_head, *rest):
    devices = lax.axis_size("dev")
    pairs = image_feats.shape[0] * devices
    small = (
        4 * pairs * pairs <= LOGIT_BUDGET
        and devices >= 8
        and devices & (devices - 1) == 0
        and image_head.shape[1] % LANES == 0
        and 2 * image_feats.shape[0] % TILE == 0
        and 2 * image_feats.shape[0] // TILE * BITS <= LANES
    )
    body = on_device_small if small else on_device_large
    return body(image_feats, text_feats, image_head, *rest)


def solution(mesh):
    placed = (P("dev", None), P("dev", None), P(), P(), P(), P(), P("dev"), P("dev"))
    return jax.shard_map(
        on_device,
        mesh=mesh,
        in_specs=placed,
        out_specs=(P(), P("dev", None), P("dev", None), P(), P()),
        check_vma=False,
    )
```

```python
import functools

import jax
import jax.numpy as jnp
from jax import lax
from jax.experimental import pallas as pl
from jax.experimental.pallas import tpu as pltpu
from jax.sharding import PartitionSpec as P


epsilon = 1e-06
LANES = 128
TILE = 8
BITS = 32
LOGIT_BUDGET = 4 << 20
SIDE_FLOPS = 1 << 26


def normalize(projected):
    length = jnp.sqrt(jnp.sum(projected * projected, axis=1, keepdims=True) + epsilon)
    return (projected / length, length)


def contract_last(a, b):
    return lax.dot_general(a, b, (((1,), (1,)), ((), ())), preferred_element_type=jnp.float32)


def backward_rows(grad_unit, unit_vec, length, weights):
    inner = jnp.sum(unit_vec * grad_unit, axis=1, keepdims=True)
    grad_proj = ((grad_unit - unit_vec * inner) / length).astype(jnp.bfloat16)
    return contract_last(grad_proj, weights).astype(jnp.bfloat16)


def on_device_large(
    image_feats, text_feats, image_head, text_head, log_scale, logit_bias, image_group, text_group
):
    img_unit, img_length = normalize(
        jnp.dot(image_feats, image_head, preferred_element_type=jnp.float32)
    )
    txt_unit, txt_length = normalize(
        jnp.dot(text_feats, text_head, preferred_element_type=jnp.float32)
    )
    img_emb = img_unit.astype(jnp.bfloat16)
    txt_emb = txt_unit.astype(jnp.bfloat16)
    logit_scale = jnp.exp(log_scale)
    pairs = image_feats.shape[0] * lax.axis_size("dev")
    emb_piece = lax.all_gather(jnp.stack([img_emb, txt_emb]), "dev", axis=1, tiled=True)
    id_piece = lax.all_gather(jnp.stack([image_group, text_group]), "dev", axis=1, tiled=True)

    def side(emb, others, group, other_group):
        cosine = contract_last(emb, others)
        label = jnp.where(group[:, None] == other_group[None, :], 1.0, -1.0).astype(jnp.float32)
        margin = label * (logit_scale * cosine + logit_bias)
        slopes = -label * jax.nn.sigmoid(-margin)
        grad = logit_scale * jnp.dot(
            slopes.astype(jnp.bfloat16), others, preferred_element_type=jnp.float32
        )
        return cosine, margin, slopes, grad

    cosine, margin, slopes, grad_img = side(img_emb, emb_piece[1], image_group, id_piece[1])
    local_sums = jnp.stack(
        [jnp.sum(jax.nn.softplus(-margin)), jnp.sum(slopes * cosine), jnp.sum(slopes)]
    )
    grad_txt = side(txt_emb, emb_piece[0], text_group, id_piece[0])[3]
    totals = lax.psum(local_sums, "dev")
    return (
        totals[0] / pairs,
        backward_rows(grad_img, img_unit, img_length, image_head),
        backward_rows(grad_txt, txt_unit, txt_length, text_head),
        logit_scale * totals[1] / pairs,
        totals[2] / pairs,
    )


def project_kernel(
    image_ids, text_ids, image_feats, text_feats, image_head, text_head,
    payload, img_kept, txt_kept,
    image_kept, text_kept, frame, image_rows, text_rows,
    image_marks, text_marks, head_sems, sems,
):
    rows, width = image_feats.shape[0], image_head.shape[1]
    depth, chunks = image_head.shape[0], head_sems.shape[1]
    step = depth // chunks
    odd = lax.rem(lax.axis_index("dev"), 2) == 1
    small = [
        pltpu.make_async_copy(source, target, sems.at[i])
        for i, (source, target) in enumerate(
            (
                (image_feats, image_rows),
                (text_feats, text_rows),
                (image_ids, image_marks),
                (text_ids, text_marks),
            )
        )
    ]
    large = [
        [
            pltpu.make_async_copy(
                head.at[pl.ds(i * step, step)], kept.at[pl.ds(i * step, step)], head_sems.at[side, i]
            )
            for i in range(chunks)
        ]
        for side, (head, kept) in enumerate(((image_head, image_kept), (text_head, text_kept)))
    ]
    small[0].start()
    for copy in large[0]:
        copy.start()
    for copy in small[1:]:
        copy.start()
    for copy in large[1]:
        copy.start()

    units = []
    sides = (
        (image_rows, image_kept, img_kept),
        (text_rows, text_kept, txt_kept),
    )
    for side, (feats, kept, out) in enumerate(sides):
        small[side].wait()
        projected = jnp.zeros((rows, width), jnp.float32)
        for i, copy in enumerate(large[side]):
            copy.wait()
            part = slice(i * step, (i + 1) * step)
            projected += jnp.dot(feats[:, part], kept[part], preferred_element_type=jnp.float32)
        unit, length = normalize(projected)
        out[:, :width] = unit
        out[:, width:] = jnp.broadcast_to(length, (rows, LANES))
        units.append(unit)
    frame[:rows] = jnp.where(odd, units[1], units[0])
    frame[rows:] = jnp.where(odd, units[0], units[1])
    groups = 2 * rows // TILE
    for block in range(width // LANES):
        columns = slice(block * LANES, (block + 1) * LANES)
        for group in range(groups):
            part = frame[group * TILE : (group + 1) * TILE, columns]
            payload[block * groups + group] = part.astype(jnp.bfloat16)

    for copy in small[2:]:
        copy.wait()
    position = lax.broadcasted_iota(jnp.int32, (TILE, LANES), 0)
    lane = lax.broadcasted_iota(jnp.int32, (TILE, LANES), 1)
    position += TILE * (lane // BITS)
    ids = jnp.zeros((TILE, LANES), jnp.int32)
    for row in range(rows):
        image_id, text_id = image_marks[row], text_marks[row]
        ids = jnp.where(position == row, jnp.where(odd, text_id, image_id), ids)
        ids = jnp.where(position == rows + row, jnp.where(odd, image_id, text_id), ids)
    bits = lax.shift_right_logical(ids, lane & (BITS - 1)) & 1
    payload[payload.shape[0] - 1] = jnp.where(bits == 1, 1.0, -1.0).astype(jnp.bfloat16)


def hop_orders(devices):
    bits = [1 << level for level in reversed(range(1, devices.bit_length() - 1))]
    first, rest = bits[:1], bits[1:]
    return first + rest, first + [rest[2], rest[0], rest[1]]


def parity(number, bits):
    return sum((number >> level) & 1 for level in range(bits)) % 2


def slot_of(apart, order):
    hops = [int(apart & bit != 0) for bit in order]
    return hops[-1] + 2 * hops[-2] + 4 * sum(hop << level for level, hop in enumerate(hops[:-2]))


def frame_of(ref, slot, block, groups, lane):
    if (block + 1) * groups < ref.shape[1]:
        tiles = ref[slot, block * groups : (block + 1) * groups].astype(jnp.float32)
        return tiles.reshape(groups * TILE, LANES)
    packed = ref[slot, ref.shape[1] - 1].astype(jnp.float32)
    turned = [packed] + [
        pltpu.roll(packed, LANES - group * BITS, axis=1) for group in range(1, groups)
    ]
    return jnp.where(lane < BITS, jnp.concatenate(turned, axis=0), 0.0)


def pair_terms(cosine, matches, scale, bias):
    label = jnp.where(matches > BITS - 1.0, 1.0, -1.0)
    negative = -label * (scale * cosine + bias)
    decay = jnp.exp(-jnp.abs(negative))
    inverse = 1.0 / (1.0 + decay)
    slopes = -label * jnp.where(negative >= 0.0, inverse, decay * inverse)
    return negative, decay, slopes


def loss_kernel(chips, pairs, orders, *refs):
    mine_pieces, other_pieces = refs[:4], refs[4:8]
    (
        img_kept, txt_kept, scalars, image_head, text_head,
        loss, grad_images, grad_texts, grad_scale, grad_bias,
        img_frames, txt_frames, cosines, matches, image_out, text_out,
        loss_out, scale_out, bias_out, sems,
    ) = refs[8:]
    rows, width = img_kept.shape[0], img_kept.shape[1] - LANES
    frame_rows, groups = 2 * rows, 2 * rows // TILE
    blocks = width // LANES + 1
    device = lax.axis_index("dev")
    odd, chip = lax.rem(device, 2), device // 2
    depth = chips.bit_length() - 1
    scale, bias = scalars[0, :1, :1], scalars[1, :1, :1]

    position = lax.broadcasted_iota(jnp.int32, (frame_rows, LANES), 0)
    lane = lax.broadcasted_iota(jnp.int32, (frame_rows, LANES), 1)
    from_mine = (position < rows) == (odd == 0)

    def assemble(held, passed):
        for apart in range(chips):
            target = jnp.bitwise_xor(chip, apart)
            flip = apart.bit_count() % 2 == 1
            (mine, slot), (other, other_slot) = (
                (pieces[slot % 4], slot // 4)
                for pieces, slot in (
                    (mine_pieces, slot_of(2 * apart, held)),
                    (other_pieces, slot_of(2 * apart, passed)),
                )
            )
            for block in range(blocks):
                columns = slice(block * LANES, (block + 1) * LANES)
                a = frame_of(mine, slot, block, groups, lane)
                b = frame_of(other, other_slot, block, groups, lane)
                a, b = (b, a) if flip else (a, b)
                img_frames[target, :, columns] = jnp.where(from_mine, a, b).astype(jnp.bfloat16)
                txt_frames[target, :, columns] = jnp.where(from_mine, b, a).astype(jnp.bfloat16)

    kind = parity(device, depth + 1)
    pl.when(kind == 0)(functools.partial(assemble, orders[0], orders[1]))
    pl.when(kind == 1)(functools.partial(assemble, orders[1], orders[0]))
    flat = (chips * frame_rows, blocks * LANES)
    img_all, txt_all = img_frames[...].reshape(flat), txt_frames[...].reshape(flat)

    img_emb, txt_emb = img_all[:, :width], txt_all[:, :width]
    img_ids, txt_ids = img_all[:, width:], txt_all[:, width:]
    cosines[...] = contract_last(img_emb, txt_emb)
    matches[...] = contract_last(img_ids, txt_ids)

    def own_rows(rows_of_chip, late):
        return jnp.where(late, rows_of_chip[rows:], rows_of_chip[:rows])

    here = pl.ds(pl.multiple_of(chip * frame_rows, TILE), frame_rows)
    own_txt_ids = own_rows(txt_frames[chip, :, width:].astype(jnp.float32), odd == 0)
    txt_unit = txt_kept[:, :width].astype(jnp.bfloat16)
    projected = []
    for kept, cosine, match, others in (
        (img_kept, own_rows(cosines[here], odd == 1), own_rows(matches[here], odd == 1), txt_emb),
        (
            txt_kept,
            contract_last(txt_unit, img_emb),
            contract_last(own_txt_ids.astype(jnp.bfloat16), img_ids),
            img_emb,
        ),
    ):
        unit, length = kept[:, :width], kept[:, width : width + 1]
        slopes = pair_terms(cosine, match, scale, bias)[2].astype(jnp.bfloat16)
        grad = scale * jnp.dot(slopes, others, preferred_element_type=jnp.float32)
        inner = jnp.sum(unit * grad, axis=1, keepdims=True)
        projected.append(((grad - unit * inner) / length).astype(jnp.bfloat16))

    def back(side, head, out, at=slice(None)):
        out[:, at] = contract_last(projected[side], head[at]).astype(jnp.bfloat16)

    def gather_sums(low, high, sums):
        for strip in range(low, high, TILE):
            strip_rows = slice(strip, strip + TILE)
            cosine = cosines[strip_rows]
            negative, decay, slopes = pair_terms(cosine, matches[strip_rows], scale, bias)
            terms = (jnp.maximum(negative, 0.0) + jnp.log1p(decay), slopes * cosine, slopes)
            sums = tuple(total + term for total, term in zip(sums, terms))
        return sums

    sums = (jnp.zeros((TILE, pairs), jnp.float32),) * 3
    copies = [
        pltpu.make_async_copy(image_out, grad_images, sems.at[0]),
        pltpu.make_async_copy(text_out, grad_texts, sems.at[1]),
        pltpu.make_async_copy(loss_out, loss, sems.at[2]),
        pltpu.make_async_copy(scale_out, grad_scale, sems.at[3]),
        pltpu.make_async_copy(bias_out, grad_bias, sems.at[4]),
    ]
    back(0, image_head, image_out)
    copies[0].start()
    back(1, text_head, text_out)
    copies[1].start()
    sums = gather_sums(0, pairs, sums)
    totals = [jnp.sum(total, keepdims=True) / pairs for total in sums]
    loss_out[0] = totals[0][0, 0]
    scale_out[0] = (scale * totals[1])[0, 0]
    bias_out[0] = totals[2][0, 0]
    for copy in copies[2:]:
        copy.start()
    for copy in copies:
        copy.wait()


def fetch_kernel(image_head, text_head, new, image_held, text_held, sems):
    copies = [
        pltpu.make_async_copy(image_head, image_held, sems.at[0]),
        pltpu.make_async_copy(text_head, text_held, sems.at[1]),
    ]
    for copy in copies:
        copy.start()
    for copy in copies:
        copy.wait()


def scalar_kernel(log_scale, logit_bias, payload, scalars):
    scalars[0] = jnp.exp(jnp.full(scalars.shape[1:], log_scale[0], jnp.float32))
    scalars[1] = jnp.full(scalars.shape[1:], logit_bias[0], jnp.float32)


def on_device_small(
    image_feats, text_feats, image_head, text_head, log_scale, logit_bias, image_group, text_group
):
    devices = lax.axis_size("dev")
    chips = devices // 2
    rows, depth = image_feats.shape
    width = image_head.shape[1]
    blocks = width // LANES + 1
    tiles = 2 * rows // TILE * (width // LANES) + 1
    chunks = next(c for c in (1,) if depth % (c * LANES) == 0 or c == 1)
    vmem, smem, hbm = (
        pl.BlockSpec(memory_space=pltpu.VMEM),
        pl.BlockSpec(memory_space=pltpu.SMEM),
        pl.BlockSpec(memory_space=pltpu.HBM),
    )
    f32, bf16 = jnp.float32, jnp.bfloat16
    payload, img_kept, txt_kept = pl.pallas_call(
        project_kernel,
        out_shape=(
            jax.ShapeDtypeStruct((tiles, TILE, LANES), bf16),
            jax.ShapeDtypeStruct((rows, width + LANES), f32),
            jax.ShapeDtypeStruct((rows, width + LANES), f32),
        ),
        in_specs=[hbm] * 6,
        out_specs=(vmem,) * 3,
        scratch_shapes=[
            pltpu.VMEM((depth, width), bf16),
            pltpu.VMEM((depth, width), bf16),
            pltpu.VMEM((2 * rows, width), f32),
            pltpu.VMEM((rows, depth), bf16),
            pltpu.VMEM((rows, depth), bf16),
            pltpu.SMEM((rows,), jnp.int32),
            pltpu.SMEM((rows,), jnp.int32),
            pltpu.SemaphoreType.DMA((2, chunks)),
            pltpu.SemaphoreType.DMA((4,)),
        ],
        compiler_params=pltpu.CompilerParams(vmem_limit_bytes=16 << 20),
        name="project",
    )(
        *(
            pltpu.with_memory_space_constraint(array, pltpu.HBM)
            for array in (image_group, text_group, image_feats, text_feats, image_head, text_head)
        )
    )

    orders = hop_orders(devices)
    bits = devices.bit_length() - 1

    def swap(array):
        return lax.ppermute(array, "dev", [(i, i ^ 1) for i in range(devices)])

    def hop(array, level):
        pairs = [(i, i ^ orders[parity(i, bits)][level] ^ 1) for i in range(devices)]
        return lax.ppermute(array, "dev", pairs)

    scalars = pl.pallas_call(
        scalar_kernel,
        out_shape=jax.ShapeDtypeStruct((2, TILE, LANES), f32),
        in_specs=[smem, smem, pl.BlockSpec(memory_space=pl.ANY)],
        out_specs=vmem,
        cost_estimate=pl.CostEstimate(flops=SIDE_FLOPS, bytes_accessed=64, transcendentals=0),
        compiler_params=pltpu.CompilerParams(vmem_limit_bytes=1 << 20),
        name="scalars",
    )(log_scale.reshape(1), logit_bias.reshape(1), payload)

    def grow(first, level):
        early = hop(first[0], level)
        late = hop(first[1], level)
        return jnp.concatenate([early, late], axis=0)

    own = payload[None]
    one = hop(own, 0)
    one, scalars = lax.optimization_barrier((one, scalars))
    pair = jnp.concatenate([own, one], axis=0)
    two = hop(pair, 1)
    old = jnp.concatenate([pair, two], axis=0)
    new = grow((pair, two), 2)
    old_far = hop(old, 3)
    new_far = hop(new, 3)
    image_held, text_held = pl.pallas_call(
        fetch_kernel,
        out_shape=(jax.ShapeDtypeStruct((depth, width), bf16),) * 2,
        in_specs=[hbm, hbm, pl.BlockSpec(memory_space=pl.ANY)],
        out_specs=(vmem,) * 2,
        scratch_shapes=[pltpu.SemaphoreType.DMA((2,))],
        cost_estimate=pl.CostEstimate(
            flops=SIDE_FLOPS, bytes_accessed=4 * depth * width, transcendentals=0
        ),
        compiler_params=pltpu.CompilerParams(vmem_limit_bytes=8 << 20),
        name="fetch",
    )(
        pltpu.with_memory_space_constraint(image_head, pltpu.HBM),
        pltpu.with_memory_space_constraint(text_head, pltpu.HBM),
        new,
    )
    old_other = swap(old)
    new_other = swap(new)
    old_far_other = swap(old_far)
    new_far, image_held, text_held, old_other, new_other, old_far_other = lax.optimization_barrier(
        (new_far, image_held, text_held, old_other, new_other, old_far_other)
    )
    new_far_other = swap(new_far)
    pieces = (old, old_far, new, new_far, old_other, old_far_other, new_other, new_far_other)

    loss, grad_images, grad_texts, grad_scale, grad_bias = pl.pallas_call(
        functools.partial(loss_kernel, chips, rows * devices, orders),
        out_shape=(
            jax.ShapeDtypeStruct((1,), f32),
            jax.ShapeDtypeStruct((rows, depth), bf16),
            jax.ShapeDtypeStruct((rows, depth), bf16),
            jax.ShapeDtypeStruct((1,), f32),
            jax.ShapeDtypeStruct((1,), f32),
        ),
        in_specs=[vmem] * 13,
        out_specs=(hbm,) * 5,
        scratch_shapes=[pltpu.VMEM((chips, 2 * rows, blocks * LANES), bf16)] * 2
        + [pltpu.VMEM((rows * devices, rows * devices), f32)] * 2
        + [pltpu.VMEM((rows, depth), bf16)] * 2
        + [pltpu.SMEM((1,), f32)] * 3
        + [pltpu.SemaphoreType.DMA((5,))],
        compiler_params=pltpu.CompilerParams(vmem_limit_bytes=24 << 20),
        name="loss",
    )(
        *(
            pltpu.with_memory_space_constraint(array, pltpu.VMEM)
            for array in pieces
            + (img_kept, txt_kept, scalars, image_held, text_held)
        )
    )
    return (loss[0], grad_images, grad_texts, grad_scale[0], grad_bias[0])


def on_device(image_feats, text_feats, image_head, *rest):
    devices = lax.axis_size("dev")
    pairs = image_feats.shape[0] * devices
    small = (
        4 * pairs * pairs <= LOGIT_BUDGET
        and devices >= 8
        and devices & (devices - 1) == 0
        and image_head.shape[1] % LANES == 0
        and 2 * image_feats.shape[0] % TILE == 0
        and 2 * image_feats.shape[0] // TILE * BITS <= LANES
    )
    body = on_device_small if small else on_device_large
    return body(image_feats, text_feats, image_head, *rest)


def solution(mesh):
    placed = (P("dev", None), P("dev", None), P(), P(), P(), P(), P("dev"), P("dev"))
    return jax.shard_map(
        on_device,
        mesh=mesh,
        in_specs=placed,
        out_specs=(P(), P("dev", None), P("dev", None), P(), P()),
        check_vma=False,
    )
```

```python
import functools

import jax
import jax.numpy as jnp
from jax import lax
from jax.experimental import pallas as pl
from jax.experimental.pallas import tpu as pltpu
from jax.sharding import PartitionSpec as P


epsilon = 1e-06
LANES = 128
TILE = 8
BITS = 32
LOGIT_BUDGET = 4 << 20
SIDE_FLOPS = 1 << 26
HOPS = 4


def normalize(projected):
    length = jnp.sqrt(jnp.sum(projected * projected, axis=1, keepdims=True) + epsilon)
    return (projected / length, length)


def contract_last(a, b):
    return lax.dot_general(a, b, (((1,), (1,)), ((), ())), preferred_element_type=jnp.float32)


def backward_rows(grad_unit, unit_vec, length, weights):
    inner = jnp.sum(unit_vec * grad_unit, axis=1, keepdims=True)
    grad_proj = ((grad_unit - unit_vec * inner) / length).astype(jnp.bfloat16)
    return contract_last(grad_proj, weights).astype(jnp.bfloat16)


def on_device_large(
    image_feats, text_feats, image_head, text_head, log_scale, logit_bias, image_group, text_group
):
    img_unit, img_length = normalize(
        jnp.dot(image_feats, image_head, preferred_element_type=jnp.float32)
    )
    txt_unit, txt_length = normalize(
        jnp.dot(text_feats, text_head, preferred_element_type=jnp.float32)
    )
    img_emb = img_unit.astype(jnp.bfloat16)
    txt_emb = txt_unit.astype(jnp.bfloat16)
    logit_scale = jnp.exp(log_scale)
    pairs = image_feats.shape[0] * lax.axis_size("dev")
    emb_piece = lax.all_gather(jnp.stack([img_emb, txt_emb]), "dev", axis=1, tiled=True)
    id_piece = lax.all_gather(jnp.stack([image_group, text_group]), "dev", axis=1, tiled=True)

    def side(emb, others, group, other_group):
        cosine = contract_last(emb, others)
        label = jnp.where(group[:, None] == other_group[None, :], 1.0, -1.0).astype(jnp.float32)
        margin = label * (logit_scale * cosine + logit_bias)
        slopes = -label * jax.nn.sigmoid(-margin)
        grad = logit_scale * jnp.dot(
            slopes.astype(jnp.bfloat16), others, preferred_element_type=jnp.float32
        )
        return cosine, margin, slopes, grad

    cosine, margin, slopes, grad_img = side(img_emb, emb_piece[1], image_group, id_piece[1])
    local_sums = jnp.stack(
        [jnp.sum(jax.nn.softplus(-margin)), jnp.sum(slopes * cosine), jnp.sum(slopes)]
    )
    grad_txt = side(txt_emb, emb_piece[0], text_group, id_piece[0])[3]
    totals = lax.psum(local_sums, "dev")
    return (
        totals[0] / pairs,
        backward_rows(grad_img, img_unit, img_length, image_head),
        backward_rows(grad_txt, txt_unit, txt_length, text_head),
        logit_scale * totals[1] / pairs,
        totals[2] / pairs,
    )


def project_kernel(
    image_ids, text_ids, image_feats, text_feats, image_head, text_head,
    payload, img_kept, txt_kept,
    image_kept, text_kept, frame, image_rows, text_rows,
    image_marks, text_marks, head_sems, sems,
):
    rows, width = image_feats.shape[0], image_head.shape[1]
    depth, chunks = image_head.shape[0], head_sems.shape[1]
    step = depth // chunks
    odd = lax.rem(lax.axis_index("dev"), 2) == 1
    small = [
        pltpu.make_async_copy(source, target, sems.at[i])
        for i, (source, target) in enumerate(
            (
                (image_feats, image_rows),
                (text_feats, text_rows),
                (image_ids, image_marks),
                (text_ids, text_marks),
            )
        )
    ]
    large = [
        [
            pltpu.make_async_copy(
                head.at[pl.ds(i * step, step)], kept.at[pl.ds(i * step, step)], head_sems.at[side, i]
            )
            for i in range(chunks)
        ]
        for side, (head, kept) in enumerate(((image_head, image_kept), (text_head, text_kept)))
    ]
    small[0].start()
    for copy in large[0]:
        copy.start()
    for copy in small[1:]:
        copy.start()
    for copy in large[1]:
        copy.start()

    units = []
    sides = (
        (image_rows, image_kept, img_kept),
        (text_rows, text_kept, txt_kept),
    )
    for side, (feats, kept, out) in enumerate(sides):
        small[side].wait()
        projected = jnp.zeros((rows, width), jnp.float32)
        for i, copy in enumerate(large[side]):
            copy.wait()
            part = slice(i * step, (i + 1) * step)
            projected += jnp.dot(feats[:, part], kept[part], preferred_element_type=jnp.float32)
        unit, length = normalize(projected)
        out[:, :width] = unit
        out[:, width:] = jnp.broadcast_to(length, (rows, LANES))
        units.append(unit)
    frame[:rows] = jnp.where(odd, units[1], units[0])
    frame[rows:] = jnp.where(odd, units[0], units[1])
    groups = 2 * rows // TILE
    for block in range(width // LANES):
        columns = slice(block * LANES, (block + 1) * LANES)
        for group in range(groups):
            part = frame[group * TILE : (group + 1) * TILE, columns]
            payload[block * groups + group] = part.astype(jnp.bfloat16)

    for copy in small[2:]:
        copy.wait()
    position = lax.broadcasted_iota(jnp.int32, (TILE, LANES), 0)
    lane = lax.broadcasted_iota(jnp.int32, (TILE, LANES), 1)
    position += TILE * (lane // BITS)
    ids = jnp.zeros((TILE, LANES), jnp.int32)
    for row in range(rows):
        image_id, text_id = image_marks[row], text_marks[row]
        ids = jnp.where(position == row, jnp.where(odd, text_id, image_id), ids)
        ids = jnp.where(position == rows + row, jnp.where(odd, image_id, text_id), ids)
    bits = lax.shift_right_logical(ids, lane & (BITS - 1)) & 1
    payload[payload.shape[0] - 1] = jnp.where(bits == 1, 1.0, -1.0).astype(jnp.bfloat16)


def hop_orders(devices):
    bits = [1 << level for level in reversed(range(1, devices.bit_length() - 1))]
    first, rest = bits[:1], bits[1:]
    rest = rest[-1:] + rest[:-1]
    return first + rest, first + rest[::-1]


def parity(number, bits):
    return sum((number >> level) & 1 for level in range(bits)) % 2


def slot_of(apart, order):
    hops = [int(apart & bit != 0) for bit in order]
    return hops[-1] + 2 * hops[-2] + 4 * sum(hop << level for level, hop in enumerate(hops[:-2]))


def frame_of(ref, slot, block, groups, lane):
    if (block + 1) * groups < ref.shape[1]:
        tiles = ref[slot, block * groups : (block + 1) * groups].astype(jnp.float32)
        return tiles.reshape(groups * TILE, LANES)
    packed = ref[slot, ref.shape[1] - 1].astype(jnp.float32)
    turned = [packed] + [
        pltpu.roll(packed, LANES - group * BITS, axis=1) for group in range(1, groups)
    ]
    return jnp.where(lane < BITS, jnp.concatenate(turned, axis=0), 0.0)


def pair_terms(cosine, matches, scale, bias):
    label = jnp.where(matches > BITS - 1.0, 1.0, -1.0)
    negative = -label * (scale * cosine + bias)
    decay = jnp.exp(-jnp.abs(negative))
    inverse = 1.0 / (1.0 + decay)
    slopes = -label * jnp.where(negative >= 0.0, inverse, decay * inverse)
    return negative, decay, slopes


def loss_kernel(chips, pairs, orders, *refs):
    mine_pieces, other_pieces = refs[:4], refs[4:8]
    (
        img_kept, txt_kept, scalars, image_head, text_head,
        loss, grad_images, grad_texts, grad_scale, grad_bias,
        img_frames, txt_frames, cosines, matches, image_out, text_out,
        loss_out, scale_out, bias_out, sems,
    ) = refs[8:]
    rows, width = img_kept.shape[0], img_kept.shape[1] - LANES
    frame_rows, groups = 2 * rows, 2 * rows // TILE
    blocks = width // LANES + 1
    device = lax.axis_index("dev")
    odd, chip = lax.rem(device, 2), device // 2
    depth = chips.bit_length() - 1
    scale, bias = scalars[0, :1, :1], scalars[1, :1, :1]

    position = lax.broadcasted_iota(jnp.int32, (frame_rows, LANES), 0)
    lane = lax.broadcasted_iota(jnp.int32, (frame_rows, LANES), 1)
    from_mine = (position < rows) == (odd == 0)

    def assemble(held, passed):
        for apart in range(chips):
            target = jnp.bitwise_xor(chip, apart)
            flip = apart.bit_count() % 2 == 1
            (mine, slot), (other, other_slot) = (
                (pieces[slot % 4], slot // 4)
                for pieces, slot in (
                    (mine_pieces, slot_of(2 * apart, held)),
                    (other_pieces, slot_of(2 * apart, passed)),
                )
            )
            for block in range(blocks):
                columns = slice(block * LANES, (block + 1) * LANES)
                a = frame_of(mine, slot, block, groups, lane)
                b = frame_of(other, other_slot, block, groups, lane)
                a, b = (b, a) if flip else (a, b)
                img_frames[target, :, columns] = jnp.where(from_mine, a, b).astype(jnp.bfloat16)
                txt_frames[target, :, columns] = jnp.where(from_mine, b, a).astype(jnp.bfloat16)

    kind = parity(device, depth + 1)
    pl.when(kind == 0)(functools.partial(assemble, orders[0], orders[1]))
    pl.when(kind == 1)(functools.partial(assemble, orders[1], orders[0]))
    flat = (chips * frame_rows, blocks * LANES)
    img_all, txt_all = img_frames[...].reshape(flat), txt_frames[...].reshape(flat)

    img_emb, txt_emb = img_all[:, :width], txt_all[:, :width]
    img_ids, txt_ids = img_all[:, width:], txt_all[:, width:]
    cosines[...] = contract_last(img_emb, txt_emb)
    matches[...] = contract_last(img_ids, txt_ids)

    def own_rows(rows_of_chip, late):
        return jnp.where(late, rows_of_chip[rows:], rows_of_chip[:rows])

    here = pl.ds(pl.multiple_of(chip * frame_rows, TILE), frame_rows)
    own_txt_ids = own_rows(txt_frames[chip, :, width:].astype(jnp.float32), odd == 0)
    txt_unit = txt_kept[:, :width].astype(jnp.bfloat16)
    projected = []
    for kept, cosine, match, others in (
        (img_kept, own_rows(cosines[here], odd == 1), own_rows(matches[here], odd == 1), txt_emb),
        (
            txt_kept,
            contract_last(txt_unit, img_emb),
            contract_last(own_txt_ids.astype(jnp.bfloat16), img_ids),
            img_emb,
        ),
    ):
        unit, length = kept[:, :width], kept[:, width : width + 1]
        slopes = pair_terms(cosine, match, scale, bias)[2].astype(jnp.bfloat16)
        grad = scale * jnp.dot(slopes, others, preferred_element_type=jnp.float32)
        inner = jnp.sum(unit * grad, axis=1, keepdims=True)
        projected.append(((grad - unit * inner) / length).astype(jnp.bfloat16))

    def back(side, head, out, at=slice(None)):
        out[:, at] = contract_last(projected[side], head[at]).astype(jnp.bfloat16)

    def gather_sums(low, high, sums):
        for strip in range(low, high, TILE):
            strip_rows = slice(strip, strip + TILE)
            cosine = cosines[strip_rows]
            negative, decay, slopes = pair_terms(cosine, matches[strip_rows], scale, bias)
            terms = (jnp.maximum(negative, 0.0) + jnp.log1p(decay), slopes * cosine, slopes)
            sums = tuple(total + term for total, term in zip(sums, terms))
        return sums

    sums = (jnp.zeros((TILE, pairs), jnp.float32),) * 3
    copies = [
        pltpu.make_async_copy(image_out, grad_images, sems.at[0]),
        pltpu.make_async_copy(text_out, grad_texts, sems.at[1]),
        pltpu.make_async_copy(loss_out, loss, sems.at[2]),
        pltpu.make_async_copy(scale_out, grad_scale, sems.at[3]),
        pltpu.make_async_copy(bias_out, grad_bias, sems.at[4]),
    ]
    back(0, image_head, image_out)
    copies[0].start()
    back(1, text_head, text_out)
    copies[1].start()
    sums = gather_sums(0, pairs, sums)
    totals = [jnp.sum(total, keepdims=True) / pairs for total in sums]
    loss_out[0] = totals[0][0, 0]
    scale_out[0] = (scale * totals[1])[0, 0]
    bias_out[0] = totals[2][0, 0]
    for copy in copies[2:]:
        copy.start()
    for copy in copies:
        copy.wait()


def fetch_kernel(image_head, text_head, new, image_held, text_held, sems):
    copies = [
        pltpu.make_async_copy(image_head, image_held, sems.at[0]),
        pltpu.make_async_copy(text_head, text_held, sems.at[1]),
    ]
    for copy in copies:
        copy.start()
    for copy in copies:
        copy.wait()


def scalar_kernel(log_scale, logit_bias, payload, scalars):
    scalars[0] = jnp.exp(jnp.full(scalars.shape[1:], log_scale[0], jnp.float32))
    scalars[1] = jnp.full(scalars.shape[1:], logit_bias[0], jnp.float32)


def on_device_small(
    image_feats, text_feats, image_head, text_head, log_scale, logit_bias, image_group, text_group
):
    devices = lax.axis_size("dev")
    chips = devices // 2
    rows, depth = image_feats.shape
    width = image_head.shape[1]
    blocks = width // LANES + 1
    tiles = 2 * rows // TILE * (width // LANES) + 1
    chunks = next(c for c in (1,) if depth % (c * LANES) == 0 or c == 1)
    vmem, smem, hbm = (
        pl.BlockSpec(memory_space=pltpu.VMEM),
        pl.BlockSpec(memory_space=pltpu.SMEM),
        pl.BlockSpec(memory_space=pltpu.HBM),
    )
    f32, bf16 = jnp.float32, jnp.bfloat16
    payload, img_kept, txt_kept = pl.pallas_call(
        project_kernel,
        out_shape=(
            jax.ShapeDtypeStruct((tiles, TILE, LANES), bf16),
            jax.ShapeDtypeStruct((rows, width + LANES), f32),
            jax.ShapeDtypeStruct((rows, width + LANES), f32),
        ),
        in_specs=[hbm] * 6,
        out_specs=(vmem,) * 3,
        scratch_shapes=[
            pltpu.VMEM((depth, width), bf16),
            pltpu.VMEM((depth, width), bf16),
            pltpu.VMEM((2 * rows, width), f32),
            pltpu.VMEM((rows, depth), bf16),
            pltpu.VMEM((rows, depth), bf16),
            pltpu.SMEM((rows,), jnp.int32),
            pltpu.SMEM((rows,), jnp.int32),
            pltpu.SemaphoreType.DMA((2, chunks)),
            pltpu.SemaphoreType.DMA((4,)),
        ],
        compiler_params=pltpu.CompilerParams(vmem_limit_bytes=16 << 20),
        name="project",
    )(
        *(
            pltpu.with_memory_space_constraint(array, pltpu.HBM)
            for array in (image_group, text_group, image_feats, text_feats, image_head, text_head)
        )
    )

    orders = hop_orders(devices)
    bits = devices.bit_length() - 1

    def swap(array):
        return lax.ppermute(array, "dev", [(i, i ^ 1) for i in range(devices)])

    def hop(array, level):
        pairs = [(i, i ^ orders[parity(i, bits)][level] ^ 1) for i in range(devices)]
        return lax.ppermute(array, "dev", pairs)

    scalars = pl.pallas_call(
        scalar_kernel,
        out_shape=jax.ShapeDtypeStruct((2, TILE, LANES), f32),
        in_specs=[smem, smem, pl.BlockSpec(memory_space=pl.ANY)],
        out_specs=vmem,
        cost_estimate=pl.CostEstimate(flops=SIDE_FLOPS, bytes_accessed=64, transcendentals=0),
        compiler_params=pltpu.CompilerParams(vmem_limit_bytes=1 << 20),
        name="scalars",
    )(log_scale.reshape(1), logit_bias.reshape(1), payload)

    def grow(first, level):
        early = hop(first[0], level)
        late = hop(first[1], level)
        return jnp.concatenate([early, late], axis=0)

    own = payload[None]
    one = hop(own, 0)
    one, scalars = lax.optimization_barrier((one, scalars))
    pair = jnp.concatenate([own, one], axis=0)
    two = hop(pair, 1)
    old = jnp.concatenate([pair, two], axis=0)
    new = grow((pair, two), 2)
    old_far = hop(old, 3)
    new_far = hop(new, 3)
    image_held, text_held = pl.pallas_call(
        fetch_kernel,
        out_shape=(jax.ShapeDtypeStruct((depth, width), bf16),) * 2,
        in_specs=[hbm, hbm, pl.BlockSpec(memory_space=pl.ANY)],
        out_specs=(vmem,) * 2,
        scratch_shapes=[pltpu.SemaphoreType.DMA((2,))],
        cost_estimate=pl.CostEstimate(
            flops=SIDE_FLOPS, bytes_accessed=4 * depth * width, transcendentals=0
        ),
        compiler_params=pltpu.CompilerParams(vmem_limit_bytes=8 << 20),
        name="fetch",
    )(
        pltpu.with_memory_space_constraint(image_head, pltpu.HBM),
        pltpu.with_memory_space_constraint(text_head, pltpu.HBM),
        new,
    )
    old_other = swap(old)
    new_other = swap(new)
    old_far_other = swap(old_far)
    new_far, image_held, text_held, old_other, new_other, old_far_other = lax.optimization_barrier(
        (new_far, image_held, text_held, old_other, new_other, old_far_other)
    )
    new_far_other = swap(new_far)
    pieces = (old, old_far, new, new_far, old_other, old_far_other, new_other, new_far_other)

    loss, grad_images, grad_texts, grad_scale, grad_bias = pl.pallas_call(
        functools.partial(loss_kernel, chips, rows * devices, orders),
        out_shape=(
            jax.ShapeDtypeStruct((1,), f32),
            jax.ShapeDtypeStruct((rows, depth), bf16),
            jax.ShapeDtypeStruct((rows, depth), bf16),
            jax.ShapeDtypeStruct((1,), f32),
            jax.ShapeDtypeStruct((1,), f32),
        ),
        in_specs=[vmem] * 13,
        out_specs=(hbm,) * 5,
        scratch_shapes=[pltpu.VMEM((chips, 2 * rows, blocks * LANES), bf16)] * 2
        + [pltpu.VMEM((rows * devices, rows * devices), f32)] * 2
        + [pltpu.VMEM((rows, depth), bf16)] * 2
        + [pltpu.SMEM((1,), f32)] * 3
        + [pltpu.SemaphoreType.DMA((5,))],
        compiler_params=pltpu.CompilerParams(vmem_limit_bytes=24 << 20),
        name="loss",
    )(
        *(
            pltpu.with_memory_space_constraint(array, pltpu.VMEM)
            for array in pieces
            + (img_kept, txt_kept, scalars, image_held, text_held)
        )
    )
    return (loss[0], grad_images, grad_texts, grad_scale[0], grad_bias[0])


def on_device(image_feats, text_feats, image_head, *rest):
    devices = lax.axis_size("dev")
    pairs = image_feats.shape[0] * devices
    small = (
        4 * pairs * pairs <= LOGIT_BUDGET
        and devices == 2 << HOPS
        and image_head.shape[1] % LANES == 0
        and 2 * image_feats.shape[0] % TILE == 0
        and 2 * image_feats.shape[0] // TILE * BITS <= LANES
    )
    body = on_device_small if small else on_device_large
    return body(image_feats, text_feats, image_head, *rest)


def solution(mesh):
    placed = (P("dev", None), P("dev", None), P(), P(), P(), P(), P("dev"), P("dev"))
    return jax.shard_map(
        on_device,
        mesh=mesh,
        in_specs=placed,
        out_specs=(P(), P("dev", None), P("dev", None), P(), P()),
        check_vma=False,
    )
```
